256 devices in a mesh: section: 16 (over z, core), seq: 16 (over x, y).
Axes of the slice: x: 4, y: 4, z: 8, core: 2. Of those that a mesh axis runs over, the one named last changes fastest.
Arguments:
- frames_in: bfloat16 [4, 16, 128, 1152], P(None, 'seq'), may hold values from -6 to 6
- spatial_qkv: bfloat16 [16, 1152, 1728], P('section'), may hold values from -0.1875 to 0.1875
- spatial_out: bfloat16 [16, 576, 1152], P('section'), may hold values from -0.25 to 0.25
- temporal_qkv: bfloat16 [16, 1152, 1728], P('section'), may hold values from -0.1875 to 0.1875
- temporal_out: bfloat16 [16, 576, 1152], P('section'), may hold values from -0.25 to 0.25
- modulation: float32 [16, 4, 6, 1152], P('section'), may hold values from -3 to 3
Outputs:
- hidden: bfloat16 [16, 4, 16, 128, 1152], P('section', None, 'seq')
The draws below stay inside these ranges and needn't reach their ends.
All inputs are finite; a program needn't handle non-finite values.
Results may differ from the reference program's by a relative error of at most 0.015.
Values may be sent and summed in bfloat16 or wider, within the bound.
No kernel may reach another device: no remote copies, remote signals or barrier semaphores. Data moves between devices by JAX's collectives and lax.ppermute only.
A program may use at most 64 MiB of HBM per device.

```python
import math
import jax
import jax.numpy as jnp
from jax import lax

D = 1152
HEADS = 8
PATCHES = 128
SAMPLES = 4
HW = 576
FRAMES = 16
SECTIONS = 16


def level_of(stream_key, dims, cuts, low, top_value):
    gain = 1.0
    for axis_at, parts in cuts:
        steps = jax.random.uniform(jax.random.fold_in(jax.random.fold_in(stream_key, 6), axis_at), (parts,), jnp.float32, low / len(cuts), top_value / len(cuts))
        gain = gain * jnp.repeat(jnp.exp(steps), dims[axis_at] // parts).reshape((-1,) + (1,) * (len(dims) - 1 - axis_at))
    return gain


def gaussian(own_key, dims, deviation, most, shards=(), kind=jnp.bfloat16):
    level = level_of(own_key, dims, shards, -0.22, 0.18) if shards else 1.0
    array = jax.random.normal(own_key, dims, jnp.float32) * deviation * level
    return jnp.minimum(jnp.maximum(array, -most), most).astype(kind)


def setup_inputs(seed: int = 0) -> dict:
    keys = jax.random.split(jax.random.key(seed), 7)
    frames_in = gaussian(keys[0], (SAMPLES, FRAMES, PATCHES, D), 1.0, 6.0, ((1, 16),))
    spatial_qkv = gaussian(keys[1], (SECTIONS, D, 3 * HW), D ** -0.5, 0.1875, ((0, 16),))
    spatial_out = gaussian(keys[2], (SECTIONS, HW, D), HW ** -0.5, 0.25, ((0, 16),))
    temporal_qkv = gaussian(keys[3], (SECTIONS, D, 3 * HW), D ** -0.5, 0.1875, ((0, 16),))
    temporal_out = gaussian(keys[4], (SECTIONS, HW, D), HW ** -0.5, 0.25, ((0, 16),))
    modulation = gaussian(keys[5], (SECTIONS, SAMPLES, 6, D), 0.5, 3.0, ((0, 16),), jnp.float32)
    return {"frames_in": frames_in, "spatial_qkv": spatial_qkv, "spatial_out": spatial_out, "temporal_qkv": temporal_qkv, "temporal_out": temporal_out, "modulation": modulation}


def norm_modulate(residual, offset, scaling):
    average = lax.optimization_barrier(jnp.mean(residual, axis=-1, keepdims=True))
    centered = residual - average
    variance = lax.optimization_barrier(jnp.mean(centered * centered, axis=-1, keepdims=True))
    return (centered / jnp.sqrt(variance + 1e-06) * (1.0 + scaling) + offset).astype(jnp.bfloat16)

def head_rms(tensor):
    return (tensor / jnp.sqrt(lax.optimization_barrier(jnp.mean(tensor * tensor, axis=-1, keepdims=True)) + 1e-06)).astype(jnp.bfloat16)

def split_heads(projected, head_count):
    head_width = projected.shape[-1] // 3
    heads_shape = projected.shape[:-1] + (head_count, head_width // head_count)
    queries = head_rms(projected[..., :head_width].reshape(heads_shape))
    lookups = head_rms(projected[..., head_width:2 * head_width].reshape(heads_shape))
    values = projected[..., 2 * head_width:].reshape(heads_shape).astype(jnp.bfloat16)
    return (queries, lookups, values)

def merge_heads(tensor):
    return tensor.reshape(tensor.shape[:-2] + (tensor.shape[-2] * tensor.shape[-1],))

def attend(queries, lookups, values):
    queries, lookups, values = lax.optimization_barrier((queries, lookups, values))
    scores = jnp.einsum('...qhd,...khd->...hqk', queries.astype(jnp.float32), lookups.astype(jnp.float32))
    scores = scores / math.sqrt(queries.shape[-1])
    exponent = jnp.exp(scores)
    totals = lax.optimization_barrier(jnp.sum(exponent, axis=-1))
    rounded = lax.optimization_barrier(exponent.astype(jnp.bfloat16))
    mixed = jnp.einsum('...hqk,...khd->...qhd', rounded.astype(jnp.float32), values.astype(jnp.float32))
    return (mixed / jnp.swapaxes(totals, -1, -2)[..., None]).astype(jnp.bfloat16)

def reference(frames_in, spatial_qkv, spatial_out, temporal_qkv, temporal_out, modulation):
    residual = frames_in.astype(jnp.float32)
    outputs = []
    for section_index in range(SECTIONS):
        factors = modulation[section_index][:, :, None, None, :]
        normed = norm_modulate(residual, factors[:, 0], factors[:, 1])
        projected = jnp.dot(normed, spatial_qkv[section_index], preferred_element_type=jnp.float32)
        queries, lookups, values = split_heads(projected, HEADS)
        mixed = merge_heads(attend(queries, lookups, values))
        middle = residual + factors[:, 2] * jnp.dot(mixed, spatial_out[section_index], preferred_element_type=jnp.float32)
        normed = norm_modulate(middle, factors[:, 3], factors[:, 4])
        projected = jnp.dot(normed, temporal_qkv[section_index], preferred_element_type=jnp.float32)
        queries, lookups, values = split_heads(projected, HEADS)
        mixed = attend(jnp.swapaxes(queries, 1, 2), jnp.swapaxes(lookups, 1, 2), jnp.swapaxes(values, 1, 2))
        mixed = merge_heads(jnp.swapaxes(mixed, 1, 2))
        updated = middle + factors[:, 5] * jnp.dot(mixed, temporal_out[section_index], preferred_element_type=jnp.float32)
        updated = lax.optimization_barrier(updated.astype(jnp.bfloat16))
        outputs.append(updated)
        residual = updated.astype(jnp.float32)
    return jnp.stack(outputs)
```

```python
import jax
import jax.numpy as jnp
from jax import lax
from jax.experimental import pallas as pl
from jax.experimental.pallas import tpu as pltpu
from jax.sharding import PartitionSpec as P

HEADS = 8
F32 = jnp.float32
BF16 = jnp.bfloat16
EPS = 1e-06


def dot(a, b):
    return lax.dot_general(a, b, (((1,), (0,)), ((), ())), preferred_element_type=F32)


def dot_t(a, b):
    return lax.dot_general(a, b, (((1,), (1,)), ((), ())), preferred_element_type=F32)


def dot_split(a, b):
    high = a.astype(BF16)
    low = (a - high.astype(F32)).astype(BF16)
    return dot(high, b) + dot(low, b)


def norm_modulate(x, offset, scaling):
    average = jnp.mean(x, axis=-1, keepdims=True)
    centered = x - average
    variance = jnp.mean(centered * centered, axis=-1, keepdims=True)
    return (centered * lax.rsqrt(variance + EPS) * (1.0 + scaling) + offset).astype(BF16)


def head_rms(t, members, members_t, width):
    square = dot_split(t * t, members) * (1.0 / width)
    return (t * dot_split(lax.rsqrt(square + EPS), members_t)).astype(BF16)


def in_head(shape, axis, start, head, width):
    at = lax.broadcasted_iota(jnp.int32, shape, axis) + start
    return jnp.logical_and(at >= head * width, at < (head + 1) * width)


def attention(projected, patches):
    tokens, total_width = projected.shape
    hw = total_width // 3
    width = hw // HEADS
    row = lax.broadcasted_iota(jnp.int32, (hw, 128), 0)
    col = lax.broadcasted_iota(jnp.int32, (hw, 128), 1) * width
    members = jnp.where(jnp.logical_and(row >= col, row < col + width), 1.0, 0.0).astype(BF16)
    row = lax.broadcasted_iota(jnp.int32, (128, hw), 0) * width
    col = lax.broadcasted_iota(jnp.int32, (128, hw), 1)
    members_t = jnp.where(jnp.logical_and(col >= row, col < row + width), 1.0, 0.0).astype(BF16)
    queries = head_rms(projected[:, :hw], members, members_t, width)
    lookups = head_rms(projected[:, hw : 2 * hw], members, members_t, width)
    values = projected[:, 2 * hw :].astype(BF16)
    scale = width**-0.5
    if patches:
        r = lax.broadcasted_iota(jnp.int32, (tokens, tokens), 0) % patches
        c = lax.broadcasted_iota(jnp.int32, (tokens, tokens), 1) % patches
        same = r == c
    tiles = [None] * (-(-hw // 128))
    for head in range(HEADS):
        first = head * width // 128
        last = ((head + 1) * width - 1) // 128
        start, stop = first * 128, min((last + 1) * 128, hw)
        mine = in_head((1, stop - start), 1, start, head, width)
        window = jnp.where(mine, queries[:, start:stop], jnp.zeros((), BF16))
        e = jnp.exp(dot_t(window, lookups[:, start:stop]) * scale)
        if patches:
            e = jnp.where(same, e, 0.0)
        inverse = 1.0 / jnp.sum(e, axis=-1, keepdims=True)
        mixed = dot(e.astype(BF16), values[:, start:stop]) * inverse
        for tile in range(first, last + 1):
            begin, end = tile * 128, min(tile * 128 + 128, hw)
            own = in_head((1, end - begin), 1, begin, head, width)
            part = mixed[:, begin - start : end - start]
            base = 0.0 if tiles[tile] is None else tiles[tile]
            tiles[tile] = jnp.where(own, part, base)
    return jnp.concatenate(tiles, axis=1).astype(BF16)


def start_either(flag, mine, other, target, sem):
    @pl.when(flag == 0)
    def _():
        pltpu.make_async_copy(mine, target, sem).start()

    @pl.when(flag != 0)
    def _():
        pltpu.make_async_copy(other, target, sem).start()


def factors_of(flag, video, mine, other):
    return jnp.where(flag == 0, mine[0, video], other[0, video])


def spatial_part(x, factors, qkv, out, waits):
    normed = norm_modulate(x, factors[0:1], factors[1:2])
    waits[0].wait()
    mixed = attention(dot(normed, qkv[...]), 0)
    waits[1].wait()
    y = x + factors[2:3] * dot(mixed, out[...])
    return y, norm_modulate(y, factors[3:4], factors[4:5])


def head_kernel(flags, frames, arriving, mod, mod2, qkv, qkv2, out, out2, y, g, x_v, qkv_v, out_v, sems):
    pick, video = flags[0], flags[1]
    start_either(flags[2], frames.at[video], arriving, x_v, sems.at[0])
    start_either(pick, qkv.at[0], qkv2.at[0], qkv_v, sems.at[1])
    start_either(pick, out.at[0], out2.at[0], out_v, sems.at[2])
    wq = pltpu.make_async_copy(qkv.at[0], qkv_v, sems.at[1])
    wo = pltpu.make_async_copy(out.at[0], out_v, sems.at[2])
    factors = factors_of(pick, video, mod, mod2)
    pltpu.make_async_copy(arriving, x_v, sems.at[0]).wait()
    y[...], g[...] = spatial_part(x_v[...].astype(F32), factors, qkv_v, out_v, (wq, wo))


def temporal_kernel(flags, arrived, qkv, qkv2, mixed, qkv_v, sems):
    start_either(flags[0], qkv.at[0], qkv2.at[0], qkv_v, sems.at[0])
    h = arrived[...]
    pltpu.make_async_copy(qkv.at[0], qkv_v, sems.at[0]).wait()
    mixed[...] = attention(dot(h, qkv_v[...]), 8)


def joint_kernel(
    flags, returned, y_in, mod, mod2, tout, tout2, qkv, qkv2, out, out2,
    x, y, g, tout_v, qkv_v, out_v, sems,
):
    pick, video = flags[0], flags[1]
    start_either(pick, tout.at[0], tout2.at[0], tout_v, sems.at[0])
    start_either(1 - pick, qkv.at[0], qkv2.at[0], qkv_v, sems.at[1])
    start_either(1 - pick, out.at[0], out2.at[0], out_v, sems.at[2])
    wq = pltpu.make_async_copy(qkv.at[0], qkv_v, sems.at[1])
    wo = pltpu.make_async_copy(out.at[0], out_v, sems.at[2])
    factors = factors_of(pick, video, mod, mod2)
    following = factors_of(1 - pick, video, mod, mod2)
    pltpu.make_async_copy(tout.at[0], tout_v, sems.at[0]).wait()
    leaving = (y_in[...] + factors[5:6] * dot(returned[...], tout_v[...])).astype(BF16)
    x[...] = leaving
    y[...], g[...] = spatial_part(leaving.astype(F32), following, qkv_v, out_v, (wq, wo))


def tail_kernel(flags, returned, y_in, mod, mod2, tout, tout2, x, tout_v, sems):
    pick, video = flags[0], flags[1]
    start_either(pick, tout.at[0], tout2.at[0], tout_v, sems.at[0])
    factors = factors_of(pick, video, mod, mod2)
    pltpu.make_async_copy(tout.at[0], tout_v, sems.at[0]).wait()
    x[...] = (y_in[...] + factors[5:6] * dot(returned[...], tout_v[...])).astype(BF16)


SMEM = pl.BlockSpec(memory_space=pltpu.SMEM)
VMEM = pl.BlockSpec(memory_space=pltpu.VMEM)
ANY = pl.BlockSpec(memory_space=pl.ANY)


def call(kernel, name, ins, outs, scratch, sems):
    return pl.pallas_call(
        kernel,
        name=name,
        in_specs=ins,
        out_specs=[VMEM] * len(outs),
        out_shape=outs,
        scratch_shapes=scratch + [pltpu.SemaphoreType.DMA((sems,))],
        compiler_params=pltpu.CompilerParams(vmem_limit_bytes=40 * 2**20),
    )


def on_device(frames_in, spatial_qkv, spatial_out, temporal_qkv, temporal_out, modulation):
    videos, frames, patches, model = frames_in.shape
    wide, hw = spatial_qkv.shape[2], spatial_out.shape[1]
    per_core = videos // 2
    sections = lax.axis_size("section")
    ranks = lax.axis_size("seq")
    stages = sections // 2
    section = lax.axis_index("section")
    stage, core = section // 2, section % 2
    tokens = frames * patches
    share = patches // ranks

    def swapped(a):
        return lax.ppermute(a, "section", [(i, i ^ 1) for i in range(sections)])

    mod2 = swapped(modulation)
    sqkv, sqkv2 = spatial_qkv, swapped(spatial_qkv)
    sout, sout2 = spatial_out, swapped(spatial_out)
    tqkv, tqkv2 = temporal_qkv, swapped(temporal_qkv)
    tout, tout2 = temporal_out, swapped(temporal_out)
    mod = modulation
    source = frames_in.reshape(videos, tokens, model)

    x_s = jax.ShapeDtypeStruct((tokens, model), BF16)
    y_s = jax.ShapeDtypeStruct((tokens, model), F32)
    mixed_s = jax.ShapeDtypeStruct((tokens, hw), BF16)
    w_qkv = pltpu.VMEM((model, wide), BF16)
    w_out = pltpu.VMEM((hw, model), BF16)
    head = call(
        head_kernel, "head", [SMEM, ANY, ANY, VMEM, VMEM, ANY, ANY, ANY, ANY], [y_s, x_s],
        [pltpu.VMEM((tokens, model), BF16), w_qkv, w_out], 3,
    )
    temporal = call(temporal_kernel, "temporal", [SMEM, VMEM, ANY, ANY], [mixed_s], [w_qkv], 1)
    joint = call(
        joint_kernel, "joint", [SMEM, VMEM, VMEM, VMEM, VMEM] + [ANY] * 6, [x_s, y_s, x_s],
        [w_out, w_qkv, w_out], 3,
    )
    tail = call(tail_kernel, "tail", [SMEM, VMEM, VMEM, VMEM, VMEM, ANY, ANY], [x_s], [w_out], 1)

    def exchange(a):
        out = lax.all_to_all(a.reshape(ranks, share, a.shape[1]), "seq", 0, 0, tiled=True)
        return out.reshape(a.shape)

    def advance(step, carried):
        even, odd, arriving = carried
        micro = step - stage
        active = jnp.logical_and(micro >= 0, micro < per_core)
        clipped = jnp.clip(micro, 0, per_core - 1)
        slot = jnp.where(active, clipped, per_core)
        video = core * per_core + clipped
        later = jnp.where(stage == 0, 0, 1)
        first = jnp.stack([core, video, later]).astype(jnp.int32)
        second = jnp.stack([1 - core, video, later]).astype(jnp.int32)
        y, g = head(first, source, arriving, mod, mod2, sqkv, sqkv2, sout, sout2)
        (mixed,) = temporal(first, exchange(g), tqkv, tqkv2)
        x, y, g = joint(
            first, exchange(mixed), y, mod, mod2, tout, tout2, sqkv, sqkv2, sout, sout2
        )
        even = lax.dynamic_update_slice_in_dim(even, x[None], slot, 0)
        (mixed,) = temporal(second, exchange(g), tqkv, tqkv2)
        (x,) = tail(second, exchange(mixed), y, mod, mod2, tout, tout2)
        arriving = lax.ppermute(x, "section", [(i, i + 2) for i in range(sections - 2)])
        odd = lax.dynamic_update_slice_in_dim(odd, x[None], slot, 0)
        return even, odd, arriving

    kept = jnp.zeros((per_core + 1, tokens, model), BF16)
    even, odd, _ = lax.fori_loop(
        0, stages + per_core - 1, advance, (kept, kept, jnp.zeros((tokens, model), BF16))
    )
    even, odd = even[:per_core], odd[:per_core]
    own = jnp.where(core == 0, even, odd)
    other = swapped(jnp.where(core == 0, odd, even))
    low, high = jnp.where(core == 0, own, other), jnp.where(core == 0, other, own)
    hidden = jnp.concatenate([low, high], axis=0)
    return hidden.reshape((1,) + frames_in.shape)


def solution(mesh):
    placed = (
        P(None, "seq", None, None),
        P("section", None, None),
        P("section", None, None),
        P("section", None, None),
        P("section", None, None),
        P("section", None, None, None),
    )
    return jax.shard_map(
        on_device,
        mesh=mesh,
        in_specs=placed,
        out_specs=P("section", None, "seq", None, None),
        check_vma=False,
    )
```

```python
import functools

import jax
import jax.numpy as jnp
from jax import lax
from jax.experimental import pallas as pl
from jax.experimental.pallas import tpu as pltpu
from jax.sharding import PartitionSpec as P

HEADS = 8
LANES = 128
F32 = jnp.float32
BF16 = jnp.bfloat16
EPS = 1e-06


def padded(n):
    return -(-n // LANES) * LANES


def dot(a, b):
    return lax.dot_general(a, b, (((1,), (0,)), ((), ())), preferred_element_type=F32)


def dot_t(a, b):
    return lax.dot_general(a, b, (((1,), (1,)), ((), ())), preferred_element_type=F32)


def split(a):
    high = a.astype(BF16)
    return high, (a - high.astype(F32)).astype(BF16)


def norm_modulate(x, offset, scaling):
    average = jnp.mean(x, axis=-1, keepdims=True)
    centered = x - average
    variance = jnp.mean(centered * centered, axis=-1, keepdims=True)
    return (centered * lax.rsqrt(variance + EPS) * (1.0 + scaling) + offset).astype(BF16)


def in_head(shape, axis, start, head, width):
    at = lax.broadcasted_iota(jnp.int32, shape, axis) + start
    return jnp.logical_and(at >= head * width, at < (head + 1) * width)


def head_members(hw, width):
    row = lax.broadcasted_iota(jnp.int32, (hw, LANES), 0)
    col = lax.broadcasted_iota(jnp.int32, (hw, LANES), 1) * width
    tall = jnp.where(jnp.logical_and(row >= col, row < col + width), 1.0, 0.0)
    row = lax.broadcasted_iota(jnp.int32, (HEADS, hw), 0) * width
    col = lax.broadcasted_iota(jnp.int32, (HEADS, hw), 1)
    flat = jnp.where(jnp.logical_and(col >= row, col < row + width), 1.0, 0.0)
    return tall.astype(BF16), flat.astype(BF16)


def attention(projected, hw, patches):
    tokens = projected.shape[0]
    width = hw // HEADS
    begin = padded(hw)
    tall, flat = head_members(hw, width)
    queries, lookups = projected[:, :hw], projected[:, begin : begin + hw]
    values = projected[:, begin + hw : begin + 2 * hw].astype(BF16)
    high, low = split(queries * queries)
    rows = lax.rsqrt((dot(high, tall) + dot(low, tall)) * (1.0 / width) + EPS) * width**-0.5
    high, low = split(lookups * lookups)
    cols = lax.rsqrt((dot_t(flat, high) + dot_t(flat, low)) * (1.0 / width) + EPS)
    queries, lookups = queries.astype(BF16), lookups.astype(BF16)
    spans, scores = [], []
    for head in range(HEADS):
        first = head * width // LANES
        last = ((head + 1) * width - 1) // LANES
        start, stop = first * LANES, min((last + 1) * LANES, hw)
        mine = in_head((1, stop - start), 1, start, head, width)
        window = jnp.where(mine, queries[:, start:stop], jnp.zeros((), BF16))
        scores.append(dot_t(window, lookups[:, start:stop]))
        spans.append((first, last, start, stop))
    e = [jnp.exp(s * rows[:, h : h + 1] * cols[h : h + 1]) for h, s in enumerate(scores)]
    if patches:
        r = lax.broadcasted_iota(jnp.int32, (tokens, tokens), 0) % patches
        c = lax.broadcasted_iota(jnp.int32, (tokens, tokens), 1) % patches
        same = r == c
        e = [jnp.where(same, a, 0.0) for a in e]
    mixed = [dot(a.astype(BF16), values[:, s[2] : s[3]]) for a, s in zip(e, spans)]
    inverse = [1.0 / jnp.sum(a, axis=-1, keepdims=True) for a in e]
    tiles = [0.0] * (padded(hw) // LANES)
    for head, (first, last, start, stop) in enumerate(spans):
        result = mixed[head] * inverse[head]
        for tile in range(first, last + 1):
            left, right = tile * LANES, min(tile * LANES + LANES, hw)
            own = in_head((1, right - left), 1, left, head, width)
            tiles[tile] = jnp.where(own, result[:, left - start : right - start], tiles[tile])
    return jnp.concatenate(tiles, axis=1).astype(BF16)


def prepare_kernel(core, qkv, qkv2, out, out2, mod, mod2, *refs):
    even, odd, out_e, out_o, mod_e, mod_o = refs[:6]
    turned, done, sems = refs[6:8], refs[8:10], refs[10]
    hw = out.shape[0]
    gap = padded(hw) - hw
    for k in range(2):
        pick = core[0] if k == 0 else 1 - core[0]

        def begin(q, o, m):
            pltpu.make_async_copy(q.at[pl.ds(0, hw)], turned[k].at[pl.ds(0, hw)], sems.at[k, 0]).start()
            pltpu.make_async_copy(
                q.at[pl.ds(hw, 2 * hw)], turned[k].at[pl.ds(hw + gap, 2 * hw)], sems.at[k, 1]
            ).start()
            pltpu.make_async_copy(o, (out_e, out_o)[k], sems.at[k, 2]).start()
            pltpu.make_async_copy(m, (mod_e, mod_o)[k], sems.at[k, 3]).start()

        pl.when(pick == 0)(lambda: begin(qkv, out, mod))
        pl.when(pick != 0)(lambda: begin(qkv2, out2, mod2))
        turned[k][hw : hw + gap, :] = jnp.zeros((gap, qkv.shape[1]), BF16)
    back = []
    for k in range(2):
        pltpu.make_async_copy(qkv.at[pl.ds(0, hw)], turned[k].at[pl.ds(0, hw)], sems.at[k, 0]).wait()
        pltpu.make_async_copy(
            qkv.at[pl.ds(hw, 2 * hw)], turned[k].at[pl.ds(hw + gap, 2 * hw)], sems.at[k, 1]
        ).wait()
        for j in range(turned[k].shape[0] // LANES):
            done[k][:, j * LANES : (j + 1) * LANES] = turned[k][j * LANES : (j + 1) * LANES, :].T
        back.append(pltpu.make_async_copy(done[k], (even, odd)[k], sems.at[k, 4]))
        back[-1].start()
    for k in range(2):
        pltpu.make_async_copy(out, (out_e, out_o)[k], sems.at[k, 2]).wait()
        pltpu.make_async_copy(mod, (mod_e, mod_o)[k], sems.at[k, 3]).wait()
        back[k].wait()


def place_of(ids, step, per_core):
    micro = step[0] - ids[0]
    inside = jnp.logical_and(micro >= 0, micro < per_core)
    clipped = jnp.clip(micro, 0, per_core - 1)
    return ids[1] * per_core + clipped, jnp.where(inside, clipped, per_core)


def spatial_part(x, factors, qkv, out, y, g):
    normed = norm_modulate(x, factors[0:1], factors[1:2])
    mixed = attention(dot(normed, qkv[...]), out.shape[0], 0)
    middle = x + factors[2:3] * dot(mixed, out[...])
    y[...] = middle
    g[...] = norm_modulate(middle, factors[3:4], factors[4:5])


def head_kernel(per_core, ids, step, frames, arriving, mod, qkv, out, y, g, x_v, sem):
    video, _ = place_of(ids, step, per_core)

    @pl.when(ids[0] == 0)
    def _():
        pltpu.make_async_copy(frames.at[video], x_v, sem).start()

    @pl.when(ids[0] != 0)
    def _():
        pltpu.make_async_copy(arriving, x_v, sem).start()

    pltpu.make_async_copy(arriving, x_v, sem).wait()
    spatial_part(x_v[...].astype(F32), mod[video], qkv, out, y, g)


def temporal_kernel(share, arrived, qkv, mixed):
    mixed[...] = attention(dot(arrived[...], qkv[...]), mixed.shape[1], share)


def joint_kernel(
    per_core, ids, step, returned, y_in, mod, following, tout, qkv, out, kept_in,
    y, g, kept, x_v, sem,
):
    video, slot = place_of(ids, step, per_core)
    leaving = (y_in[...] + mod[video][5:6] * dot(returned[...], tout[...])).astype(BF16)
    x_v[...] = leaving
    store = pltpu.make_async_copy(x_v, kept.at[slot], sem)
    store.start()
    spatial_part(leaving.astype(F32), following[video], qkv, out, y, g)
    store.wait()


def tail_kernel(per_core, ids, step, returned, y_in, mod, tout, kept_in, x, kept, x_v, sem):
    video, slot = place_of(ids, step, per_core)
    leaving = (y_in[...] + mod[video][5:6] * dot(returned[...], tout[...])).astype(BF16)
    x_v[...] = leaving
    store = pltpu.make_async_copy(x_v, kept.at[slot], sem)
    store.start()
    x[...] = leaving
    store.wait()


SMEM = pl.BlockSpec(memory_space=pltpu.SMEM)
VMEM = pl.BlockSpec(memory_space=pltpu.VMEM)
ANY = pl.BlockSpec(memory_space=pl.ANY)


def call(kernel, name, ins, outs, specs, scratch, aliases={}):
    return pl.pallas_call(
        kernel,
        name=name,
        in_specs=ins,
        out_specs=specs,
        out_shape=outs,
        scratch_shapes=scratch,
        input_output_aliases=aliases,
        compiler_params=pltpu.CompilerParams(vmem_limit_bytes=24 * 2**20),
    )


def on_device(frames_in, spatial_qkv, spatial_out, temporal_qkv, temporal_out, modulation):
    videos, frames, patches, model = frames_in.shape
    wide, hw = spatial_qkv.shape[2], spatial_out.shape[1]
    per_core = videos // 2
    sections = lax.axis_size("section")
    ranks = lax.axis_size("seq")
    stages = sections // 2
    section = lax.axis_index("section")
    stage, core = section // 2, section % 2
    tokens = frames * patches
    share = patches // ranks
    columns = wide + padded(hw) - hw

    def swapped(a):
        return lax.ppermute(a, "section", [(i, i ^ 1) for i in range(sections)])

    shape = jax.ShapeDtypeStruct
    factors_s = shape(modulation.shape[1:], F32)
    qkv_s, out_s = shape((model, columns), BF16), shape((hw, model), BF16)
    prepare = call(
        prepare_kernel, "prepare", [SMEM] + [ANY] * 6, [qkv_s] * 2 + [out_s] * 2 + [factors_s] * 2,
        [ANY] * 6,
        [pltpu.VMEM((columns, model), BF16)] * 2 + [pltpu.VMEM((model, columns), BF16)] * 2
        + [pltpu.SemaphoreType.DMA((2, 5))],
    )
    core_id = core.reshape(1).astype(jnp.int32)
    ids = jnp.stack([stage, core]).astype(jnp.int32)
    mod2 = swapped(modulation)

    def prepared(qkv, out, rows, rows2):
        qkv2, out2 = swapped(qkv), swapped(out)
        return prepare(
            core_id, jnp.swapaxes(qkv[0], 0, 1), jnp.swapaxes(qkv2[0], 0, 1), out[0], out2[0],
            rows, rows2,
        )

    sqkv_e, sqkv_o, sout_e, sout_o, mod_e, mod_o = prepared(
        spatial_qkv, spatial_out, modulation[0], mod2[0]
    )
    tqkv_e, tqkv_o, tout_e, tout_o, _, _ = prepared(
        temporal_qkv, temporal_out, modulation[0], mod2[0]
    )
    source = frames_in.reshape(videos, tokens, model)

    x_s, y_s = shape((tokens, model), BF16), shape((tokens, model), F32)
    kept_s = shape((per_core + 1, tokens, model), BF16)
    hold = [pltpu.VMEM((tokens, model), BF16), pltpu.SemaphoreType.DMA]
    head = call(
        functools.partial(head_kernel, per_core), "head",
        [SMEM, SMEM, ANY, ANY, VMEM, VMEM, VMEM], [y_s, x_s], [VMEM, VMEM], hold,
    )
    temporal = call(
        functools.partial(temporal_kernel, share), "temporal", [VMEM, VMEM],
        shape((tokens, hw), BF16), VMEM, [],
    )
    joint = call(
        functools.partial(joint_kernel, per_core), "joint",
        [SMEM, SMEM] + [VMEM] * 7 + [ANY], [y_s, x_s, kept_s], [VMEM, VMEM, ANY], hold, {9: 2},
    )
    tail = call(
        functools.partial(tail_kernel, per_core), "tail",
        [SMEM, SMEM] + [VMEM] * 4 + [ANY], [x_s, kept_s], [VMEM, ANY], hold, {6: 1},
    )

    def exchange(a):
        out = lax.all_to_all(a.reshape(ranks, share, a.shape[1]), "seq", 0, 0, tiled=True)
        return out.reshape(a.shape)

    def advance(step, carried):
        even, odd, arriving = carried
        at = step.reshape(1)
        y, g = head(ids, at, source, arriving, mod_e, sqkv_e, sout_e)
        mixed = temporal(exchange(g), tqkv_e)
        y, g, even = joint(
            ids, at, exchange(mixed), y, mod_e, mod_o, tout_e, sqkv_o, sout_o, even
        )
        mixed = temporal(exchange(g), tqkv_o)
        x, odd = tail(ids, at, exchange(mixed), y, mod_o, tout_o, odd)
        arriving = lax.ppermute(x, "section", [(i, i + 2) for i in range(sections - 2)])
        return even, odd, arriving

    kept = jnp.zeros(kept_s.shape, BF16)
    even, odd, _ = lax.fori_loop(
        0, stages + per_core - 1, advance, (kept, kept, jnp.zeros((tokens, model), BF16))
    )
    even, odd = even[:per_core], odd[:per_core]
    own = jnp.where(core == 0, even, odd)
    other = swapped(jnp.where(core == 0, odd, even))
    low, high = jnp.where(core == 0, own, other), jnp.where(core == 0, other, own)
    hidden = jnp.concatenate([low, high], axis=0)
    return hidden.reshape((1,) + frames_in.shape)


def solution(mesh):
    placed = (
        P(None, "seq", None, None),
        P("section", None, None),
        P("section", None, None),
        P("section", None, None),
        P("section", None, None),
        P("section", None, None, None),
    )
    return jax.shard_map(
        on_device,
        mesh=mesh,
        in_specs=placed,
        out_specs=P("section", None, "seq", None, None),
        check_vma=False,
    )
```

```python
import functools

import jax
import jax.numpy as jnp
from jax import lax
from jax.experimental import pallas as pl
from jax.experimental.pallas import tpu as pltpu
from jax.sharding import PartitionSpec as P

HEADS = 8
LANES = 128
F32 = jnp.float32
BF16 = jnp.bfloat16
EPS = 1e-06


def padded(n):
    return -(-n // LANES) * LANES


def dot(a, b):
    return lax.dot_general(a, b, (((1,), (0,)), ((), ())), preferred_element_type=F32)


def dot_t(a, b):
    return lax.dot_general(a, b, (((1,), (1,)), ((), ())), preferred_element_type=F32)


def split(a):
    high = a.astype(BF16)
    return high, (a - high.astype(F32)).astype(BF16)


def norm_modulate(x, offset, scaling):
    average = jnp.mean(x, axis=-1, keepdims=True)
    centered = x - average
    variance = jnp.mean(centered * centered, axis=-1, keepdims=True)
    return (centered * lax.rsqrt(variance + EPS) * (1.0 + scaling) + offset).astype(BF16)


def in_head(shape, axis, start, head, width):
    at = lax.broadcasted_iota(jnp.int32, shape, axis) + start
    return jnp.logical_and(at >= head * width, at < (head + 1) * width)


def head_members(hw, width):
    row = lax.broadcasted_iota(jnp.int32, (hw, LANES), 0)
    col = lax.broadcasted_iota(jnp.int32, (hw, LANES), 1) * width
    tall = jnp.where(jnp.logical_and(row >= col, row < col + width), 1.0, 0.0)
    row = lax.broadcasted_iota(jnp.int32, (HEADS, hw), 0) * width
    col = lax.broadcasted_iota(jnp.int32, (HEADS, hw), 1)
    flat = jnp.where(jnp.logical_and(col >= row, col < row + width), 1.0, 0.0)
    return tall.astype(BF16), flat.astype(BF16)


def attention(projected, hw, patches):
    tokens = projected.shape[0]
    width = hw // HEADS
    begin = padded(hw)
    tall, flat = head_members(hw, width)
    queries, lookups = projected[:, :hw], projected[:, begin : begin + hw]
    values = projected[:, begin + hw : begin + 2 * hw].astype(BF16)
    high, low = split(queries * queries)
    rows = lax.rsqrt((dot(high, tall) + dot(low, tall)) * (1.0 / width) + EPS) * width**-0.5
    high, low = split(lookups * lookups)
    cols = lax.rsqrt((dot_t(flat, high) + dot_t(flat, low)) * (1.0 / width) + EPS)
    queries, lookups = queries.astype(BF16), lookups.astype(BF16)
    spans, scores = [], []
    for head in range(HEADS):
        first = head * width // LANES
        last = ((head + 1) * width - 1) // LANES
        start, stop = first * LANES, min((last + 1) * LANES, hw)
        mine = in_head((1, stop - start), 1, start, head, width)
        window = jnp.where(mine, queries[:, start:stop], jnp.zeros((), BF16))
        scores.append(dot_t(window, lookups[:, start:stop]))
        spans.append((first, last, start, stop))
    e = [jnp.exp(s * rows[:, h : h + 1] * cols[h : h + 1]) for h, s in enumerate(scores)]
    if patches:
        r = lax.broadcasted_iota(jnp.int32, (tokens, tokens), 0) % patches
        c = lax.broadcasted_iota(jnp.int32, (tokens, tokens), 1) % patches
        same = r == c
        e = [jnp.where(same, a, 0.0) for a in e]
    mixed = [dot(a.astype(BF16), values[:, s[2] : s[3]]) for a, s in zip(e, spans)]
    inverse = [1.0 / jnp.sum(a, axis=-1, keepdims=True) for a in e]
    tiles = [0.0] * (padded(hw) // LANES)
    for head, (first, last, start, stop) in enumerate(spans):
        result = mixed[head] * inverse[head]
        for tile in range(first, last + 1):
            left, right = tile * LANES, min(tile * LANES + LANES, hw)
            own = in_head((1, right - left), 1, left, head, width)
            tiles[tile] = jnp.where(own, result[:, left - start : right - start], tiles[tile])
    return jnp.concatenate(tiles, axis=1).astype(BF16)


def prepare_kernel(core, qkv, qkv2, out, out2, even, odd, out_e, out_o, *refs):
    turned, done, sems = refs[:2], refs[2:4], refs[4]
    hw, model = out.shape
    gap = padded(hw) - hw
    parts = ((0, 0, hw), (hw, hw + gap, hw), (2 * hw, 2 * hw + gap, hw))

    def piece(k, q, j):
        at, to, rows = parts[j]
        return pltpu.make_async_copy(
            q.at[pl.ds(at, rows)], turned[k].at[pl.ds(to, rows)], sems.at[k, j]
        )

    def begin(k, q, o):
        for j in range(len(parts)):
            piece(k, q, j).start()
        pltpu.make_async_copy(o, (out_e, out_o)[k], sems.at[k, 3]).start()

    for k in range(2):
        pick = core[0] if k == 0 else 1 - core[0]
        pl.when(pick == 0)(functools.partial(begin, k, qkv, out))
        pl.when(pick != 0)(functools.partial(begin, k, qkv2, out2))
        turned[k][hw : hw + gap, :] = jnp.zeros((gap, model), BF16)
    columns = turned[0].shape[0]
    halves = ((0, columns // 2 // LANES * LANES), (columns // 2 // LANES * LANES, columns))
    back = []
    for k in range(2):
        arrived = 0
        for n, (low, high) in enumerate(halves):
            while arrived < len(parts) and parts[arrived][1] < high:
                piece(k, qkv, arrived).wait()
                arrived += 1
            for j in range(low, high, LANES):
                done[k][:, j : j + LANES] = turned[k][j : j + LANES, :].T
            back.append(
                pltpu.make_async_copy(
                    done[k].at[:, pl.ds(low, high - low)],
                    (even, odd)[k].at[:, pl.ds(low, high - low)],
                    sems.at[k, 4 + n],
                )
            )
            back[-1].start()
    for k in range(2):
        pltpu.make_async_copy(out, (out_e, out_o)[k], sems.at[k, 3]).wait()
    for copy in back:
        copy.wait()


def place_of(ids, step, per_core):
    micro = step[0] - ids[0]
    inside = jnp.logical_and(micro >= 0, micro < per_core)
    clipped = jnp.clip(micro, 0, per_core - 1)
    return ids[1] * per_core + clipped, jnp.where(inside, clipped, per_core)


def spatial_part(x, factors, qkv, out, y, g):
    normed = norm_modulate(x, factors[0:1], factors[1:2])
    mixed = attention(dot(normed, qkv[...]), out.shape[0], 0)
    middle = x + factors[2:3] * dot(mixed, out[...])
    y[...] = middle
    g[...] = norm_modulate(middle, factors[3:4], factors[4:5])


def first_kernel(per_core, ids, frames, mod, qkv, out, y, g):
    video = ids[1] * per_core
    spatial_part(frames[video].astype(F32), mod[video], qkv, out, y, g)


def head_kernel(per_core, ids, step, frames, arriving, mod, qkv, out, y, g, x_v, sem):
    video, _ = place_of(ids, step, per_core)

    @pl.when(ids[0] == 0)
    def _():
        pltpu.make_async_copy(frames.at[video], x_v, sem).start()

    @pl.when(ids[0] != 0)
    def _():
        pltpu.make_async_copy(arriving, x_v, sem).start()

    pltpu.make_async_copy(arriving, x_v, sem).wait()
    spatial_part(x_v[...].astype(F32), mod[video], qkv, out, y, g)


def temporal_kernel(share, arrived, qkv, mixed):
    mixed[...] = attention(dot(arrived[...], qkv[...]), mixed.shape[1], share)


def joint_kernel(
    per_core, ids, step, returned, y_in, mod, following, tout, qkv, out, kept_in,
    y, g, kept, x_v, sem,
):
    video, slot = place_of(ids, step, per_core)
    leaving = (y_in[...] + mod[video][5:6] * dot(returned[...], tout[...])).astype(BF16)
    x_v[...] = leaving
    store = pltpu.make_async_copy(x_v, kept.at[slot], sem)
    store.start()
    spatial_part(leaving.astype(F32), following[video], qkv, out, y, g)
    store.wait()


def tail_kernel(
    per_core, ids, step, returned, y_in, mod, tout, kept_in, x, kept, following, x_v, sem
):
    following[0] = step[0] + 1
    video, slot = place_of(ids, step, per_core)
    leaving = (y_in[...] + mod[video][5:6] * dot(returned[...], tout[...])).astype(BF16)
    x_v[...] = leaving
    store = pltpu.make_async_copy(x_v, kept.at[slot], sem)
    store.start()
    x[...] = leaving
    store.wait()


SMEM = pl.BlockSpec(memory_space=pltpu.SMEM)
VMEM = pl.BlockSpec(memory_space=pltpu.VMEM)
ANY = pl.BlockSpec(memory_space=pl.ANY)
HBM = pl.BlockSpec(memory_space=pltpu.HBM)


def call(kernel, name, ins, outs, specs, scratch, aliases={}, limit=24):
    return pl.pallas_call(
        kernel,
        name=name,
        in_specs=ins,
        out_specs=specs,
        out_shape=outs,
        scratch_shapes=scratch,
        input_output_aliases=aliases,
        compiler_params=pltpu.CompilerParams(vmem_limit_bytes=limit * 2**20),
    )


def on_device(frames_in, spatial_qkv, spatial_out, temporal_qkv, temporal_out, modulation):
    videos, frames, patches, model = frames_in.shape
    wide, hw = spatial_qkv.shape[2], spatial_out.shape[1]
    per_core = videos // 2
    sections = lax.axis_size("section")
    ranks = lax.axis_size("seq")
    stages = sections // 2
    section = lax.axis_index("section")
    stage, core = section // 2, section % 2
    tokens = frames * patches
    share = patches // ranks
    columns = wide + padded(hw) - hw

    def swapped(a):
        return lax.ppermute(a, "section", [(i, i ^ 1) for i in range(sections)])

    shape = jax.ShapeDtypeStruct
    qkv_s, out_s = shape((model, columns), BF16), shape((hw, model), BF16)
    prepare = call(
        prepare_kernel, "prepare", [SMEM] + [HBM] * 4, [qkv_s] * 2 + [out_s] * 2, [ANY] * 4,
        [pltpu.VMEM((columns, model), BF16)] * 2 + [pltpu.VMEM((model, columns), BF16)] * 2
        + [pltpu.SemaphoreType.DMA((2, 6))],
        limit=60,
    )
    chain = (stage + core) % 2
    core_id = core.reshape(1).astype(jnp.int32)
    ids = jnp.stack([stage, chain]).astype(jnp.int32)
    mod = modulation[0]
    mod2 = swapped(mod)
    mod_e, mod_o = jnp.where(core == 0, mod, mod2), jnp.where(core == 0, mod2, mod)

    def prepared(qkv, out, core_id):
        qkv2, out2 = swapped(qkv), swapped(out)
        return prepare(
            core_id, jnp.swapaxes(qkv[0], 0, 1), jnp.swapaxes(qkv2[0], 0, 1), out[0], out2[0]
        )

    sqkv_e, sqkv_o, sout_e, sout_o = prepared(spatial_qkv, spatial_out, core_id)
    source = frames_in.reshape(videos, tokens, model)

    x_s, y_s = shape((tokens, model), BF16), shape((tokens, model), F32)
    kept_s = shape((per_core + 1, tokens, model), BF16)
    hold = [pltpu.VMEM((tokens, model), BF16), pltpu.SemaphoreType.DMA]
    first = call(
        functools.partial(first_kernel, per_core), "first", [SMEM] + [VMEM] * 4,
        [y_s, x_s], [VMEM, VMEM], [],
    )
    head = call(
        functools.partial(head_kernel, per_core), "head",
        [SMEM, SMEM, ANY, ANY, VMEM, VMEM, VMEM], [y_s, x_s], [VMEM, VMEM], hold,
    )
    temporal = call(
        functools.partial(temporal_kernel, share), "temporal", [VMEM, VMEM],
        shape((tokens, hw), BF16), VMEM, [],
    )
    joint = call(
        functools.partial(joint_kernel, per_core), "joint",
        [SMEM, SMEM] + [VMEM] * 7 + [ANY], [y_s, x_s, kept_s], [VMEM, VMEM, ANY], hold, {9: 2},
    )
    tail = call(
        functools.partial(tail_kernel, per_core), "tail",
        [SMEM, SMEM] + [VMEM] * 4 + [ANY], [x_s, kept_s, shape((1,), jnp.int32)],
        [VMEM, ANY, SMEM], hold, {6: 1},
    )

    def exchange(a):
        out = lax.all_to_all(a.reshape(ranks, share, a.shape[1]), "seq", 0, 0, tiled=True)
        return out.reshape(a.shape)

    kept = jnp.zeros(kept_s.shape, BF16)
    y, g = first(ids, source, mod_e, sqkv_e, sout_e)
    g, core_id = lax.optimization_barrier((g, core_id))
    tqkv_e, tqkv_o, tout_e, tout_o = prepared(temporal_qkv, temporal_out, core_id)

    def middle(at, even, y, g):
        mixed = temporal(exchange(g), tqkv_e)
        y, g, even = joint(
            ids, at, exchange(mixed), y, mod_e, mod_o, tout_e, sqkv_o, sout_o, even
        )
        return even, y, exchange(temporal(exchange(g), tqkv_o))

    def advance(step, carried):
        odd, even, y, returned = carried
        x, odd, at = tail(ids, step.reshape(1), returned, y, mod_o, tout_o, odd)
        onward = [(i, (i + 2) ^ 1) for i in range(sections - 2)]
        arriving = lax.ppermute(x, "section", onward)
        y, g = head(ids, at, source, arriving, mod_e, sqkv_e, sout_e)
        return odd, *middle(at, even, y, g)

    last = stages + per_core - 2
    carried = kept, *middle(jnp.zeros((1,), jnp.int32), kept, y, g)
    odd, even, y, returned = lax.fori_loop(0, last, advance, carried)
    _, odd, _ = tail(
        ids, jnp.full((1,), last, jnp.int32), returned, y, mod_o, tout_o, odd
    )
    even, odd = even[:per_core], odd[:per_core]
    own = jnp.where(core == 0, even, odd)
    other = swapped(jnp.where(core == 0, odd, even))
    low, high = jnp.where(chain == 0, own, other), jnp.where(chain == 0, other, own)
    hidden = jnp.concatenate([low, high], axis=0)
    return hidden.reshape((1,) + frames_in.shape)


def solution(mesh):
    placed = (
        P(None, "seq", None, None),
        P("section", None, None),
        P("section", None, None),
        P("section", None, None),
        P("section", None, None),
        P("section", None, None, None),
    )
    return jax.shard_map(
        on_device,
        mesh=mesh,
        in_specs=placed,
        out_specs=P("section", None, "seq", None, None),
        check_vma=False,
    )
```

```python
import functools

import jax
import jax.numpy as jnp
from jax import lax
from jax.experimental import pallas as pl
from jax.experimental.pallas import tpu as pltpu
from jax.sharding import PartitionSpec as P

HEADS = 8
LANES = 128
F32 = jnp.float32
BF16 = jnp.bfloat16
EPS = 1e-06


def padded(n):
    return -(-n // LANES) * LANES


def dot(a, b):
    return lax.dot_general(a, b, (((1,), (0,)), ((), ())), preferred_element_type=F32)


def dot_t(a, b):
    return lax.dot_general(a, b, (((1,), (1,)), ((), ())), preferred_element_type=F32)


def split(a):
    high = a.astype(BF16)
    return high, (a - high.astype(F32)).astype(BF16)


def norm_modulate(x, offset, scaling):
    average = jnp.mean(x, axis=-1, keepdims=True)
    centered = x - average
    variance = jnp.mean(centered * centered, axis=-1, keepdims=True)
    return (centered * lax.rsqrt(variance + EPS) * (1.0 + scaling) + offset).astype(BF16)


def in_head(shape, axis, start, head, width):
    at = lax.broadcasted_iota(jnp.int32, shape, axis) + start
    return jnp.logical_and(at >= head * width, at < (head + 1) * width)


def head_members(hw, width):
    row = lax.broadcasted_iota(jnp.int32, (hw, LANES), 0)
    col = lax.broadcasted_iota(jnp.int32, (hw, LANES), 1) * width
    tall = jnp.where(jnp.logical_and(row >= col, row < col + width), 1.0, 0.0)
    row = lax.broadcasted_iota(jnp.int32, (HEADS, hw), 0) * width
    col = lax.broadcasted_iota(jnp.int32, (HEADS, hw), 1)
    flat = jnp.where(jnp.logical_and(col >= row, col < row + width), 1.0, 0.0)
    return tall.astype(BF16), flat.astype(BF16)


def attention(projected, hw, patches):
    tokens = projected.shape[0]
    width = hw // HEADS
    begin = padded(hw)
    tall, flat = head_members(hw, width)
    queries, lookups = projected[:, :hw], projected[:, begin : begin + hw]
    values = projected[:, begin + hw : begin + 2 * hw].astype(BF16)
    high, low = split(queries * queries)
    rows = lax.rsqrt((dot(high, tall) + dot(low, tall)) * (1.0 / width) + EPS) * width**-0.5
    high, low = split(lookups * lookups)
    cols = lax.rsqrt((dot_t(flat, high) + dot_t(flat, low)) * (1.0 / width) + EPS)
    queries, lookups = queries.astype(BF16), lookups.astype(BF16)
    spans, scores = [], []
    for head in range(HEADS):
        first = head * width // LANES
        last = ((head + 1) * width - 1) // LANES
        start, stop = first * LANES, min((last + 1) * LANES, hw)
        mine = in_head((1, stop - start), 1, start, head, width)
        window = jnp.where(mine, queries[:, start:stop], jnp.zeros((), BF16))
        scores.append(dot_t(window, lookups[:, start:stop]))
        spans.append((first, last, start, stop))
    e = [jnp.exp(s * rows[:, h : h + 1] * cols[h : h + 1]) for h, s in enumerate(scores)]
    if patches:
        r = lax.broadcasted_iota(jnp.int32, (tokens, tokens), 0) % patches
        c = lax.broadcasted_iota(jnp.int32, (tokens, tokens), 1) % patches
        same = r == c
        e = [jnp.where(same, a, 0.0) for a in e]
    mixed = [dot(a.astype(BF16), values[:, s[2] : s[3]]) for a, s in zip(e, spans)]
    inverse = [1.0 / jnp.sum(a, axis=-1, keepdims=True) for a in e]
    tiles = [0.0] * (padded(hw) // LANES)
    for head, (first, last, start, stop) in enumerate(spans):
        result = mixed[head] * inverse[head]
        for tile in range(first, last + 1):
            left, right = tile * LANES, min(tile * LANES + LANES, hw)
            own = in_head((1, right - left), 1, left, head, width)
            tiles[tile] = jnp.where(own, result[:, left - start : right - start], tiles[tile])
    return jnp.concatenate(tiles, axis=1).astype(BF16)


def prepare_kernel(core, qkv, qkv2, out, out2, even, odd, out_e, out_o, *refs):
    turned, done, sems = refs[:2], refs[2:4], refs[4]
    hw, model = out.shape
    gap = padded(hw) - hw
    parts = ((0, 0, hw), (hw, hw + gap, hw), (2 * hw, 2 * hw + gap, hw))

    def piece(k, q, j):
        at, to, rows = parts[j]
        return pltpu.make_async_copy(
            q.at[pl.ds(at, rows)], turned[k].at[pl.ds(to, rows)], sems.at[k, j]
        )

    def begin(k, q, o):
        for j in range(len(parts)):
            piece(k, q, j).start()
        pltpu.make_async_copy(o, (out_e, out_o)[k], sems.at[k, 3]).start()

    for k in range(2):
        pick = core[0] if k == 0 else 1 - core[0]
        pl.when(pick == 0)(functools.partial(begin, k, qkv, out))
        pl.when(pick != 0)(functools.partial(begin, k, qkv2, out2))
        turned[k][hw : hw + gap, :] = jnp.zeros((gap, model), BF16)
    columns = turned[0].shape[0]
    halves = ((0, columns // 2 // LANES * LANES), (columns // 2 // LANES * LANES, columns))
    back = []
    for k in range(2):
        arrived = 0
        for n, (low, high) in enumerate(halves):
            while arrived < len(parts) and parts[arrived][1] < high:
                piece(k, qkv, arrived).wait()
                arrived += 1
            for j in range(low, high, LANES):
                done[k][:, j : j + LANES] = turned[k][j : j + LANES, :].T
            back.append(
                pltpu.make_async_copy(
                    done[k].at[:, pl.ds(low, high - low)],
                    (even, odd)[k].at[:, pl.ds(low, high - low)],
                    sems.at[k, 4 + n],
                )
            )
            back[-1].start()
    for k in range(2):
        pltpu.make_async_copy(out, (out_e, out_o)[k], sems.at[k, 3]).wait()
    for copy in back:
        copy.wait()


def place_of(ids, step, per_core):
    micro = step[0] - ids[0]
    inside = jnp.logical_and(micro >= 0, micro < per_core)
    clipped = jnp.clip(micro, 0, per_core - 1)
    return inside, ids[1] * per_core + clipped, clipped


def spatial_part(x, factors, qkv, out, y, g, ready=None):
    normed = norm_modulate(x, factors[0:1], factors[1:2])
    if ready is not None:
        ready()
    mixed = attention(dot(normed, qkv[...]), out.shape[0], 0)
    middle = x + factors[2:3] * dot(mixed, out[...])
    y[...] = middle
    g[...] = norm_modulate(middle, factors[3:4], factors[4:5])


def head_kernel(
    per_core, ids, step, frames, arriving, mod, qkv, out, y, g, x_v, qkv_v, out_v, sems
):
    inside, video, _ = place_of(ids, step, per_core)

    @pl.when(inside)
    def _():
        @pl.when(ids[0] == 0)
        def _():
            pltpu.make_async_copy(frames.at[video], x_v, sems.at[0]).start()

        @pl.when(ids[0] != 0)
        def _():
            pltpu.make_async_copy(arriving, x_v, sems.at[0]).start()

        weights = (
            pltpu.make_async_copy(qkv, qkv_v, sems.at[1]),
            pltpu.make_async_copy(out, out_v, sems.at[2]),
        )
        for copy in weights:
            copy.start()

        def ready():
            for copy in weights:
                copy.wait()

        pltpu.make_async_copy(arriving, x_v, sems.at[0]).wait()
        spatial_part(x_v[...].astype(F32), mod[video], qkv_v, out_v, y, g, ready)


def temporal_kernel(per_core, share, ids, step, arrived, qkv, mixed):
    inside, _, _ = place_of(ids, step, per_core)

    @pl.when(inside)
    def _():
        mixed[...] = attention(dot(arrived[...], qkv[...]), mixed.shape[1], share)


def joint_kernel(
    per_core, ids, step, returned, y_in, mod, following, tout, qkv, out, kept_in,
    y, g, kept, x_v, sem,
):
    inside, video, slot = place_of(ids, step, per_core)

    @pl.when(inside)
    def _():
        leaving = (y_in[...] + mod[video][5:6] * dot(returned[...], tout[...])).astype(BF16)
        x_v[...] = leaving
        store = pltpu.make_async_copy(x_v, kept.at[slot], sem)
        store.start()
        spatial_part(leaving.astype(F32), following[video], qkv, out, y, g)
        store.wait()


def tail_kernel(per_core, ids, step, returned, y_in, mod, tout, kept_in, x, kept, x_v, sem):
    inside, video, slot = place_of(ids, step, per_core)

    @pl.when(inside)
    def _():
        leaving = (y_in[...] + mod[video][5:6] * dot(returned[...], tout[...])).astype(BF16)
        x_v[...] = leaving
        store = pltpu.make_async_copy(x_v, kept.at[slot], sem)
        store.start()
        x[...] = leaving
        store.wait()


SMEM = pl.BlockSpec(memory_space=pltpu.SMEM)
VMEM = pl.BlockSpec(memory_space=pltpu.VMEM)
ANY = pl.BlockSpec(memory_space=pl.ANY)
HBM = pl.BlockSpec(memory_space=pltpu.HBM)


def call(kernel, name, ins, outs, specs, scratch, aliases={}, limit=14):
    return pl.pallas_call(
        kernel,
        name=name,
        in_specs=ins,
        out_specs=specs,
        out_shape=outs,
        scratch_shapes=scratch,
        input_output_aliases=aliases,
        compiler_params=pltpu.CompilerParams(vmem_limit_bytes=limit * 2**20),
    )


def on_device(frames_in, spatial_qkv, spatial_out, temporal_qkv, temporal_out, modulation):
    videos, frames, patches, model = frames_in.shape
    wide, hw = spatial_qkv.shape[2], spatial_out.shape[1]
    per_core = videos // 2
    sections = lax.axis_size("section")
    ranks = lax.axis_size("seq")
    stages = sections // 2
    section = lax.axis_index("section")
    stage, core = section // 2, section % 2
    tokens = frames * patches
    share = patches // ranks
    columns = wide + padded(hw) - hw

    def swapped(a):
        return lax.ppermute(a, "section", [(i, i ^ 1) for i in range(sections)])

    shape = jax.ShapeDtypeStruct
    qkv_s, out_s = shape((model, columns), BF16), shape((hw, model), BF16)
    prepare = call(
        prepare_kernel, "prepare", [SMEM] + [HBM] * 4, [qkv_s] * 2 + [out_s] * 2,
        [ANY] * 2 + [VMEM] * 2,
        [pltpu.VMEM((columns, model), BF16)] * 2 + [pltpu.VMEM((model, columns), BF16)] * 2
        + [pltpu.SemaphoreType.DMA((2, 6))],
        limit=60,
    )
    chain = (stage + core) % 2
    core_id = core.reshape(1).astype(jnp.int32)
    ids = jnp.stack([stage, chain]).astype(jnp.int32)
    def prepared(qkv, out, qkv2, out2):
        return prepare(
            core_id, jnp.swapaxes(qkv[0], 0, 1), jnp.swapaxes(qkv2[0], 0, 1), out[0], out2[0]
        )

    mod = modulation[0]
    mod2, sqkv2, sout2 = swapped(mod), swapped(spatial_qkv), swapped(spatial_out)
    tqkv, tout, mod2, sqkv2, sout2 = lax.optimization_barrier(
        (temporal_qkv, temporal_out, mod2, sqkv2, sout2)
    )
    mod_e, mod_o = jnp.where(core == 0, mod, mod2), jnp.where(core == 0, mod2, mod)
    tqkv2, tout2 = swapped(tqkv), swapped(tout)
    sqkv_e, sqkv_o, sout_e, sout_o = prepared(spatial_qkv, spatial_out, sqkv2, sout2)
    tqkv_e, tqkv_o, tout_e, tout_o = prepared(tqkv, tout, tqkv2, tout2)
    source = frames_in.reshape(videos, tokens, model)

    x_s, y_s = shape((tokens, model), BF16), shape((tokens, model), F32)
    kept_s = shape((per_core, tokens, model), BF16)
    hold = [pltpu.VMEM((tokens, model), BF16), pltpu.SemaphoreType.DMA]
    head = call(
        functools.partial(head_kernel, per_core), "head",
        [SMEM, SMEM, ANY, ANY, VMEM, ANY, ANY], [y_s, x_s], [VMEM, VMEM],
        [
            pltpu.VMEM((tokens, model), BF16), pltpu.VMEM((model, columns), BF16),
            pltpu.VMEM((hw, model), BF16), pltpu.SemaphoreType.DMA((3,)),
        ],
    )
    temporal = call(
        functools.partial(temporal_kernel, per_core, share), "temporal",
        [SMEM, SMEM, VMEM, VMEM], shape((tokens, hw), BF16), VMEM, [],
    )
    joint = call(
        functools.partial(joint_kernel, per_core), "joint",
        [SMEM, SMEM] + [VMEM] * 7 + [ANY], [y_s, x_s, kept_s], [VMEM, VMEM, ANY], hold, {9: 2},
    )
    tail = call(
        functools.partial(tail_kernel, per_core), "tail",
        [SMEM, SMEM] + [VMEM] * 4 + [ANY], [x_s, kept_s], [VMEM, ANY], hold, {6: 1},
    )

    def exchange(a):
        out = lax.all_to_all(a.reshape(ranks, share, a.shape[1]), "seq", 0, 0, tiled=True)
        return out.reshape(a.shape)

    def section_pair(at, even, odd, arriving):
        y, g = head(ids, at, source, arriving, mod_e, sqkv_e, sout_e)
        mixed = temporal(ids, at, exchange(g), tqkv_e)
        y, g, even = joint(
            ids, at, exchange(mixed), y, mod_e, mod_o, tout_e, sqkv_o, sout_o, even
        )
        mixed = temporal(ids, at, exchange(g), tqkv_o)
        x, odd = tail(ids, at, exchange(mixed), y, mod_o, tout_o, odd)
        return even, odd, x

    onward = [(i, (i + 2) ^ 1) for i in range(sections - 2)]

    def advance(step, carried):
        even, odd, x = section_pair(step.reshape(1), *carried)
        return even, odd, lax.ppermute(x, "section", onward)

    kept = jnp.zeros(kept_s.shape, BF16)
    last = stages + per_core - 2
    carried = lax.fori_loop(0, last, advance, (kept, kept, jnp.zeros((tokens, model), BF16)))
    even, odd, _ = section_pair(jnp.full((1,), last, jnp.int32), *carried)
    own = jnp.where(core == 0, even, odd)
    other = swapped(jnp.where(core == 0, odd, even))
    low, high = jnp.where(chain == 0, own, other), jnp.where(chain == 0, other, own)
    hidden = jnp.concatenate([low, high], axis=0)
    return hidden.reshape((1,) + frames_in.shape)


def solution(mesh):
    placed = (
        P(None, "seq", None, None),
        P("section", None, None),
        P("section", None, None),
        P("section", None, None),
        P("section", None, None),
        P("section", None, None, None),
    )
    return jax.shard_map(
        on_device,
        mesh=mesh,
        in_specs=placed,
        out_specs=P("section", None, "seq", None, None),
        check_vma=False,
    )
```

```python
import functools

import jax
import jax.numpy as jnp
from jax import lax
from jax.experimental import pallas as pl
from jax.experimental.pallas import tpu as pltpu
from jax.sharding import PartitionSpec as P

HEADS = 8
LANES = 128
F32 = jnp.float32
BF16 = jnp.bfloat16
EPS = 1e-06


def padded(n):
    return -(-n // LANES) * LANES


def dot(a, b):
    return lax.dot_general(a, b, (((1,), (0,)), ((), ())), preferred_element_type=F32)


def dot_t(a, b):
    return lax.dot_general(a, b, (((1,), (1,)), ((), ())), preferred_element_type=F32)


def split(a):
    high = a.astype(BF16)
    return high, (a - high.astype(F32)).astype(BF16)


def norm_modulate(x, offset, scaling):
    average = jnp.mean(x, axis=-1, keepdims=True)
    centered = x - average
    variance = jnp.mean(centered * centered, axis=-1, keepdims=True)
    return (centered * lax.rsqrt(variance + EPS) * (1.0 + scaling) + offset).astype(BF16)


def in_head(shape, axis, start, head, width):
    at = lax.broadcasted_iota(jnp.int32, shape, axis) + start
    return jnp.logical_and(at >= head * width, at < (head + 1) * width)


def head_members(hw, width):
    row = lax.broadcasted_iota(jnp.int32, (hw, LANES), 0)
    col = lax.broadcasted_iota(jnp.int32, (hw, LANES), 1) * width
    tall = jnp.where(jnp.logical_and(row >= col, row < col + width), 1.0, 0.0)
    row = lax.broadcasted_iota(jnp.int32, (HEADS, hw), 0) * width
    col = lax.broadcasted_iota(jnp.int32, (HEADS, hw), 1)
    flat = jnp.where(jnp.logical_and(col >= row, col < row + width), 1.0, 0.0)
    return tall.astype(BF16), flat.astype(BF16)


def attention(projected, hw, patches):
    tokens = projected.shape[0]
    width = hw // HEADS
    begin = padded(hw)
    tall, flat = head_members(hw, width)
    queries, lookups = projected[:, :hw], projected[:, begin : begin + hw]
    values = projected[:, begin + hw : begin + 2 * hw].astype(BF16)
    high, low = split(queries * queries)
    rows = lax.rsqrt((dot(high, tall) + dot(low, tall)) * (1.0 / width) + EPS) * width**-0.5
    high, low = split(lookups * lookups)
    cols = lax.rsqrt((dot_t(flat, high) + dot_t(flat, low)) * (1.0 / width) + EPS)
    queries, lookups = queries.astype(BF16), lookups.astype(BF16)
    spans, scores = [], []
    for head in range(HEADS):
        first = head * width // LANES
        last = ((head + 1) * width - 1) // LANES
        start, stop = first * LANES, min((last + 1) * LANES, hw)
        mine = in_head((1, stop - start), 1, start, head, width)
        window = jnp.where(mine, queries[:, start:stop], jnp.zeros((), BF16))
        scores.append(dot_t(window, lookups[:, start:stop]))
        spans.append((first, last, start, stop))
    e = [jnp.exp(s * rows[:, h : h + 1] * cols[h : h + 1]) for h, s in enumerate(scores)]
    if patches:
        r = lax.broadcasted_iota(jnp.int32, (tokens, tokens), 0) % patches
        c = lax.broadcasted_iota(jnp.int32, (tokens, tokens), 1) % patches
        same = r == c
        e = [jnp.where(same, a, 0.0) for a in e]
    mixed = [dot(a.astype(BF16), values[:, s[2] : s[3]]) for a, s in zip(e, spans)]
    inverse = [1.0 / jnp.sum(a, axis=-1, keepdims=True) for a in e]
    tiles = [0.0] * (padded(hw) // LANES)
    for head, (first, last, start, stop) in enumerate(spans):
        result = mixed[head] * inverse[head]
        for tile in range(first, last + 1):
            left, right = tile * LANES, min(tile * LANES + LANES, hw)
            own = in_head((1, right - left), 1, left, head, width)
            tiles[tile] = jnp.where(own, result[:, left - start : right - start], tiles[tile])
    return jnp.concatenate(tiles, axis=1).astype(BF16)


def prepare_kernel(core, qkv, qkv2, out, out2, even, odd, out_e, out_o, *refs):
    turned, done, sems = refs[:2], refs[2:4], refs[4]
    hw, model = out.shape
    gap = padded(hw) - hw
    parts = ((0, 0, hw), (hw, hw + gap, hw), (2 * hw, 2 * hw + gap, hw))

    def piece(k, q, j):
        at, to, rows = parts[j]
        return pltpu.make_async_copy(
            q.at[pl.ds(at, rows)], turned[k].at[pl.ds(to, rows)], sems.at[k, j]
        )

    def begin(k, q, o):
        for j in range(len(parts)):
            piece(k, q, j).start()
        pltpu.make_async_copy(o, (out_e, out_o)[k], sems.at[k, 3]).start()

    for k in range(2):
        pick = core[0] if k == 0 else 1 - core[0]
        pl.when(pick == 0)(functools.partial(begin, k, qkv, out))
        pl.when(pick != 0)(functools.partial(begin, k, qkv2, out2))
        turned[k][hw : hw + gap, :] = jnp.zeros((gap, model), BF16)
    columns = turned[0].shape[0]
    halves = ((0, columns // 2 // LANES * LANES), (columns // 2 // LANES * LANES, columns))
    back = []
    for k in range(2):
        arrived = 0
        for n, (low, high) in enumerate(halves):
            while arrived < len(parts) and parts[arrived][1] < high:
                piece(k, qkv, arrived).wait()
                arrived += 1
            for j in range(low, high, LANES):
                done[k][:, j : j + LANES] = turned[k][j : j + LANES, :].T
            back.append(
                pltpu.make_async_copy(
                    done[k].at[:, pl.ds(low, high - low)],
                    (even, odd)[k].at[:, pl.ds(low, high - low)],
                    sems.at[k, 4 + n],
                )
            )
            back[-1].start()
    for k in range(2):
        pltpu.make_async_copy(out, (out_e, out_o)[k], sems.at[k, 3]).wait()
    for copy in back:
        copy.wait()


def place_of(ids, step, per_core):
    micro = step[0] - ids[0]
    inside = jnp.logical_and(micro >= 0, micro < per_core)
    clipped = jnp.clip(micro, 0, per_core - 1)
    return inside, ids[1] * per_core + clipped, clipped


def spatial_part(x, factors, qkv, out, y, g, ready=None):
    normed = norm_modulate(x, factors[0:1], factors[1:2])
    if ready is not None:
        ready()
    mixed = attention(dot(normed, qkv[...]), out.shape[0], 0)
    middle = x + factors[2:3] * dot(mixed, out[...])
    y[...] = middle
    g[...] = norm_modulate(middle, factors[3:4], factors[4:5])


def tick_kernel(step, g_in, now, following, g):
    now[0] = step[0]
    following[0] = step[0] + 1


def first_kernel(per_core, ids, frames, mod, qkv, out, y, g):
    video = ids[1] * per_core

    @pl.when(ids[0] == 0)
    def _():
        spatial_part(frames[video].astype(F32), mod[video], qkv, out, y, g)


def cross_kernel(
    per_core, stages, ids, step, returned, y_in, mod_p, mod, tout_p, qkv, out, frames, kept_in,
    y, g, kept, x_v, new_v, sems,
):
    inside, video, _ = place_of(ids, step, per_core)
    micro = jnp.where(ids[0] == 0, step[0] - stages, step[0] - ids[0])
    finishing = jnp.logical_and(micro >= 0, micro < per_core)
    slot = jnp.clip(micro, 0, per_core - 1)

    @pl.when(finishing)
    def _():
        factor = mod_p[ids[1] * per_core + slot][5:6]
        x_v[...] = (y_in[...] + factor * dot(returned[...], tout_p[...])).astype(BF16)
        pltpu.make_async_copy(x_v, kept.at[slot], sems.at[0]).start()

    @pl.when(inside)
    def _():
        @pl.when(ids[0] == 0)
        def _():
            copy = pltpu.make_async_copy(frames.at[video], new_v, sems.at[1])
            copy.start()
            copy.wait()

        x = jnp.where(ids[0] == 0, new_v[...], x_v[...])
        spatial_part(x.astype(F32), mod[video], qkv, out, y, g)

    @pl.when(finishing)
    def _():
        pltpu.make_async_copy(x_v, kept.at[slot], sems.at[0]).wait()


def temporal_kernel(per_core, share, ids, step, arrived, qkv, mixed):
    inside, _, _ = place_of(ids, step, per_core)

    @pl.when(inside)
    def _():
        mixed[...] = attention(dot(arrived[...], qkv[...]), mixed.shape[1], share)


def joint_kernel(
    per_core, ids, step, returned, y_in, mod, following, tout, qkv, out, kept_in,
    y, g, kept, x_v, sem,
):
    inside, video, slot = place_of(ids, step, per_core)

    @pl.when(inside)
    def _():
        leaving = (y_in[...] + mod[video][5:6] * dot(returned[...], tout[...])).astype(BF16)
        x_v[...] = leaving
        store = pltpu.make_async_copy(x_v, kept.at[slot], sem)
        store.start()
        spatial_part(leaving.astype(F32), following[video], qkv, out, y, g)
        store.wait()


def tail_kernel(per_core, ids, step, returned, y_in, mod, tout, kept_in, kept, x_v, sem):
    inside, video, slot = place_of(ids, step, per_core)

    @pl.when(inside)
    def _():
        leaving = (y_in[...] + mod[video][5:6] * dot(returned[...], tout[...])).astype(BF16)
        x_v[...] = leaving
        store = pltpu.make_async_copy(x_v, kept.at[slot], sem)
        store.start()
        store.wait()


SMEM = pl.BlockSpec(memory_space=pltpu.SMEM)
VMEM = pl.BlockSpec(memory_space=pltpu.VMEM)
ANY = pl.BlockSpec(memory_space=pl.ANY)
HBM = pl.BlockSpec(memory_space=pltpu.HBM)


def call(kernel, name, ins, outs, specs, scratch, aliases={}, limit=14):
    return pl.pallas_call(
        kernel,
        name=name,
        in_specs=ins,
        out_specs=specs,
        out_shape=outs,
        scratch_shapes=scratch,
        input_output_aliases=aliases,
        compiler_params=pltpu.CompilerParams(vmem_limit_bytes=limit * 2**20),
    )


def on_device(frames_in, spatial_qkv, spatial_out, temporal_qkv, temporal_out, modulation):
    videos, frames, patches, model = frames_in.shape
    wide, hw = spatial_qkv.shape[2], spatial_out.shape[1]
    per_core = videos // 2
    sections = lax.axis_size("section")
    ranks = lax.axis_size("seq")
    stages = sections // 2
    section = lax.axis_index("section")
    stage, core = section // 2, section % 2
    tokens = frames * patches
    share = patches // ranks
    columns = wide + padded(hw) - hw

    def swapped(a):
        return lax.ppermute(a, "section", [(i, i ^ 1) for i in range(sections)])

    shape = jax.ShapeDtypeStruct
    qkv_s, out_s = shape((model, columns), BF16), shape((hw, model), BF16)
    prepare = call(
        prepare_kernel, "prepare", [SMEM] + [HBM] * 4, [qkv_s] * 2 + [out_s] * 2,
        [ANY] * 2 + [VMEM] * 2,
        [pltpu.VMEM((columns, model), BF16)] * 2 + [pltpu.VMEM((model, columns), BF16)] * 2
        + [pltpu.SemaphoreType.DMA((2, 6))],
        limit=60,
    )
    chain = (stage + core) % 2
    core_id = core.reshape(1).astype(jnp.int32)
    ids = jnp.stack([stage, chain]).astype(jnp.int32)
    def prepared(qkv, out, qkv2, out2):
        return prepare(
            core_id, jnp.swapaxes(qkv[0], 0, 1), jnp.swapaxes(qkv2[0], 0, 1), out[0], out2[0]
        )

    mod = modulation[0]
    mod2, sqkv2, sout2 = swapped(mod), swapped(spatial_qkv), swapped(spatial_out)
    tqkv, tout, mod2, sqkv2, sout2 = lax.optimization_barrier(
        (temporal_qkv, temporal_out, mod2, sqkv2, sout2)
    )
    mod_e, mod_o = jnp.where(core == 0, mod, mod2), jnp.where(core == 0, mod2, mod)
    tqkv2, tout2 = swapped(tqkv), swapped(tout)
    sqkv_e, sqkv_o, sout_e, sout_o = prepared(spatial_qkv, spatial_out, sqkv2, sout2)
    source = frames_in.reshape(videos, tokens, model)

    x_s, y_s = shape((tokens, model), BF16), shape((tokens, model), F32)
    kept_s = shape((per_core, tokens, model), BF16)
    hold = [pltpu.VMEM((tokens, model), BF16), pltpu.SemaphoreType.DMA]
    at_s = shape((1,), jnp.int32)
    tick = call(
        tick_kernel, "tick", [SMEM, ANY], [at_s, at_s, x_s], [SMEM, SMEM, ANY], [], {1: 2}
    )
    first = call(
        functools.partial(first_kernel, per_core), "first", [SMEM] + [VMEM] * 4, [y_s, x_s],
        [VMEM, VMEM], [],
    )
    cross = call(
        functools.partial(cross_kernel, per_core, stages), "cross",
        [SMEM, SMEM] + [VMEM] * 7 + [ANY, ANY], [y_s, x_s, kept_s], [VMEM, VMEM, ANY],
        [pltpu.VMEM((tokens, model), BF16)] * 2 + [pltpu.SemaphoreType.DMA((2,))], {10: 2},
    )
    temporal = call(
        functools.partial(temporal_kernel, per_core, share), "temporal",
        [SMEM, SMEM, VMEM, VMEM], shape((tokens, hw), BF16), VMEM, [],
    )
    joint = call(
        functools.partial(joint_kernel, per_core), "joint",
        [SMEM, SMEM] + [VMEM] * 7 + [ANY], [y_s, x_s, kept_s], [VMEM, VMEM, ANY], hold, {9: 2},
    )
    tail = call(
        functools.partial(tail_kernel, per_core), "tail",
        [SMEM, SMEM] + [VMEM] * 4 + [ANY], [kept_s], [ANY], hold, {6: 0},
    )

    def exchange(a):
        out = lax.all_to_all(a.reshape(ranks, share, a.shape[1]), "seq", 0, 0, tiled=True)
        return out.reshape(a.shape)

    def sections_of(at, even, y, g):
        mixed = temporal(ids, at, exchange(g), tqkv_e)
        y, g, even = joint(
            ids, at, exchange(mixed), y, mod_e, mod_o, tout_e, sqkv_o, sout_o, even
        )
        return even, y, g

    onward = [(i, ((i + 2) % sections) ^ 1) for i in range(sections)]
    back = [(j, i) for i, j in onward]

    def advance(carried):
        step, even, odd, y, g = carried
        now, following, g = tick(step, g)
        even, y, g = sections_of(now, even, y, g)
        y = lax.ppermute(y, "section", onward)
        mixed = lax.ppermute(temporal(ids, now, exchange(g), tqkv_o), "section", onward)
        y, g, odd = cross(
            ids, following, exchange(mixed), y, mod_p, mod_e, tout_p, sqkv_e, sout_e, source, odd
        )
        return following, even, odd, y, g

    kept = jnp.zeros(kept_s.shape, BF16)
    last = stages + per_core - 2
    y, g = first(ids, source, mod_e, sqkv_e, sout_e)
    tqkv2, g = lax.optimization_barrier((tqkv2, g))
    tqkv_e, tqkv_o, tout_e, tout_o = prepared(tqkv, tout, tqkv2, tout2)
    before = [(i, (i + 2) % sections) for i in range(1, sections, 2)]
    tout_p = lax.ppermute(temporal_out[0], "section", before)
    tout_p, tout_o = lax.optimization_barrier((tout_p, tout_o))
    tout_p2 = lax.ppermute(tout_p, "section", [(i, i - 1) for i in range(1, sections, 2)])
    tout_p = jnp.where(core == 0, tout_p2, tout_p)
    mod_p = lax.ppermute(mod_o, "section", [(i, (i + 2) % sections) for i in range(sections)])
    start = jnp.zeros((1,), jnp.int32)
    at, even, odd, y, g = lax.while_loop(
        lambda carried: carried[0][0] < last, advance, (start, kept, kept, y, g)
    )
    odd = lax.ppermute(odd, "section", back)
    even, y, g = sections_of(at, even, y, g)
    mixed = temporal(ids, at, exchange(g), tqkv_o)
    (odd,) = tail(ids, at, exchange(mixed), y, mod_o, tout_o, odd)
    own = jnp.where(core == 0, even, odd)
    other = swapped(jnp.where(core == 0, odd, even))
    low, high = jnp.where(chain == 0, own, other), jnp.where(chain == 0, other, own)
    hidden = jnp.concatenate([low, high], axis=0)
    return hidden.reshape((1,) + frames_in.shape)


def solution(mesh):
    placed = (
        P(None, "seq", None, None),
        P("section", None, None),
        P("section", None, None),
        P("section", None, None),
        P("section", None, None),
        P("section", None, None, None),
    )
    return jax.shard_map(
        on_device,
        mesh=mesh,
        in_specs=placed,
        out_specs=P("section", None, "seq", None, None),
        check_vma=False,
    )
```

```python
import functools

import jax
import jax.numpy as jnp
from jax import lax
from jax.experimental import pallas as pl
from jax.experimental.pallas import tpu as pltpu
from jax.sharding import PartitionSpec as P

HEADS = 8
LANES = 128
F32 = jnp.float32
BF16 = jnp.bfloat16
EPS = 1e-06


def padded(n):
    return -(-n // LANES) * LANES


def dot(a, b):
    return lax.dot_general(a, b, (((1,), (0,)), ((), ())), preferred_element_type=F32)


def dot_t(a, b):
    return lax.dot_general(a, b, (((1,), (1,)), ((), ())), preferred_element_type=F32)


def split(a):
    high = a.astype(BF16)
    return high, (a - high.astype(F32)).astype(BF16)


def norm_modulate(x, offset, scaling):
    average = jnp.mean(x, axis=-1, keepdims=True)
    centered = x - average
    variance = jnp.mean(centered * centered, axis=-1, keepdims=True)
    return (centered * lax.rsqrt(variance + EPS) * (1.0 + scaling) + offset).astype(BF16)


def in_head(shape, axis, start, head, width):
    at = lax.broadcasted_iota(jnp.int32, shape, axis) + start
    return jnp.logical_and(at >= head * width, at < (head + 1) * width)


def head_members(hw, width):
    row = lax.broadcasted_iota(jnp.int32, (hw, LANES), 0)
    col = lax.broadcasted_iota(jnp.int32, (hw, LANES), 1) * width
    tall = jnp.where(jnp.logical_and(row >= col, row < col + width), 1.0, 0.0)
    row = lax.broadcasted_iota(jnp.int32, (HEADS, hw), 0) * width
    col = lax.broadcasted_iota(jnp.int32, (HEADS, hw), 1)
    flat = jnp.where(jnp.logical_and(col >= row, col < row + width), 1.0, 0.0)
    return tall.astype(BF16), flat.astype(BF16)


def attention(projected, hw, patches):
    tokens = projected.shape[0]
    width = hw // HEADS
    begin = padded(hw)
    tall, flat = head_members(hw, width)
    queries, lookups = projected[:, :hw], projected[:, begin : begin + hw]
    values = projected[:, begin + hw : begin + 2 * hw].astype(BF16)
    high, low = split(queries * queries)
    rows = lax.rsqrt((dot(high, tall) + dot(low, tall)) * (1.0 / width) + EPS) * width**-0.5
    high, low = split(lookups * lookups)
    cols = lax.rsqrt((dot_t(flat, high) + dot_t(flat, low)) * (1.0 / width) + EPS)
    queries, lookups = queries.astype(BF16), lookups.astype(BF16)
    spans, scores = [], []
    for head in range(HEADS):
        first = head * width // LANES
        last = ((head + 1) * width - 1) // LANES
        start, stop = first * LANES, min((last + 1) * LANES, hw)
        mine = in_head((1, stop - start), 1, start, head, width)
        window = jnp.where(mine, queries[:, start:stop], jnp.zeros((), BF16))
        scores.append(dot_t(window, lookups[:, start:stop]))
        spans.append((first, last, start, stop))
    e = [jnp.exp(s * rows[:, h : h + 1] * cols[h : h + 1]) for h, s in enumerate(scores)]
    if patches:
        r = lax.broadcasted_iota(jnp.int32, (tokens, tokens), 0) % patches
        c = lax.broadcasted_iota(jnp.int32, (tokens, tokens), 1) % patches
        same = r == c
        e = [jnp.where(same, a, 0.0) for a in e]
    mixed = [dot(a.astype(BF16), values[:, s[2] : s[3]]) for a, s in zip(e, spans)]
    inverse = [1.0 / jnp.sum(a, axis=-1, keepdims=True) for a in e]
    tiles = [0.0] * (padded(hw) // LANES)
    for head, (first, last, start, stop) in enumerate(spans):
        result = mixed[head] * inverse[head]
        for tile in range(first, last + 1):
            left, right = tile * LANES, min(tile * LANES + LANES, hw)
            own = in_head((1, right - left), 1, left, head, width)
            tiles[tile] = jnp.where(own, result[:, left - start : right - start], tiles[tile])
    return jnp.concatenate(tiles, axis=1).astype(BF16)


def prepare_kernel(core, qkv, qkv2, out, out2, even, odd, out_e, out_o, *refs):
    turned, done, sems = refs[:2], refs[2:4], refs[4]
    hw, model = out.shape
    gap = padded(hw) - hw
    parts = ((0, 0, hw), (hw, hw + gap, hw), (2 * hw, 2 * hw + gap, hw))

    def piece(k, q, j):
        at, to, rows = parts[j]
        return pltpu.make_async_copy(
            q.at[pl.ds(at, rows)], turned[k].at[pl.ds(to, rows)], sems.at[k, j]
        )

    def begin(k, q, o):
        for j in range(len(parts)):
            piece(k, q, j).start()
        pltpu.make_async_copy(o, (out_e, out_o)[k], sems.at[k, 3]).start()

    for k in range(2):
        pick = core[0] if k == 0 else 1 - core[0]
        pl.when(pick == 0)(functools.partial(begin, k, qkv, out))
        pl.when(pick != 0)(functools.partial(begin, k, qkv2, out2))
        turned[k][hw : hw + gap, :] = jnp.zeros((gap, model), BF16)
    columns = turned[0].shape[0]
    halves = ((0, columns // 2 // LANES * LANES), (columns // 2 // LANES * LANES, columns))
    back = []
    for k in range(2):
        arrived = 0
        for n, (low, high) in enumerate(halves):
            while arrived < len(parts) and parts[arrived][1] < high:
                piece(k, qkv, arrived).wait()
                arrived += 1
            for j in range(low, high, LANES):
                done[k][:, j : j + LANES] = turned[k][j : j + LANES, :].T
            back.append(
                pltpu.make_async_copy(
                    done[k].at[:, pl.ds(low, high - low)],
                    (even, odd)[k].at[:, pl.ds(low, high - low)],
                    sems.at[k, 4 + n],
                )
            )
            back[-1].start()
    for k in range(2):
        pltpu.make_async_copy(out, (out_e, out_o)[k], sems.at[k, 3]).wait()
    for copy in back:
        copy.wait()


def place_of(flags, per_core, late=0):
    micro = flags[2] - late - flags[0]
    inside = jnp.logical_and(micro >= 0, micro < per_core)
    clipped = jnp.clip(micro, 0, per_core - 1)
    return inside, flags[1] * per_core + clipped, clipped


def spatial_part(x, factors, qkv, out, y, g, ready=None):
    normed = norm_modulate(x, factors[0:1], factors[1:2])
    if ready is not None:
        ready()
    mixed = attention(dot(normed, qkv[...]), out.shape[0], 0)
    middle = x + factors[2:3] * dot(mixed, out[...])
    y[...] = middle
    g[...] = norm_modulate(middle, factors[3:4], factors[4:5])


def tick_kernel(flags, g_in, following, g):
    following[0] = flags[0]
    following[1] = flags[1]
    following[2] = flags[2] + 1


def first_kernel(per_core, flags, frames, mod, qkv, out, y, g):
    video = flags[1] * per_core

    @pl.when(flags[0] == 0)
    def _():
        spatial_part(frames[video].astype(F32), mod[video], qkv, out, y, g)


def cross_kernel(
    per_core, stages, flags, returned, y_in, mod_p, mod, tout_p, qkv, out, frames, kept_in,
    y, g, kept, x_v, new_v, sems,
):
    inside, video, _ = place_of(flags, per_core)
    micro = jnp.where(flags[0] == 0, flags[2] - stages, flags[2] - flags[0])
    finishing = jnp.logical_and(micro >= 0, micro < per_core)
    slot = jnp.clip(micro, 0, per_core - 1)

    @pl.when(finishing)
    def _():
        factor = mod_p[flags[1] * per_core + slot][5:6]
        x_v[...] = (y_in[...] + factor * dot(returned[...], tout_p[...])).astype(BF16)
        pltpu.make_async_copy(x_v, kept.at[slot], sems.at[0]).start()

    @pl.when(inside)
    def _():
        @pl.when(flags[0] == 0)
        def _():
            copy = pltpu.make_async_copy(frames.at[video], new_v, sems.at[1])
            copy.start()
            copy.wait()

        x = jnp.where(flags[0] == 0, new_v[...], x_v[...])
        spatial_part(x.astype(F32), mod[video], qkv, out, y, g)

    @pl.when(finishing)
    def _():
        pltpu.make_async_copy(x_v, kept.at[slot], sems.at[0]).wait()


def temporal_kernel(share, arrived, qkv, mixed):
    mixed[...] = attention(dot(arrived[...], qkv[...]), mixed.shape[1], share)


def joint_kernel(
    per_core, late, flags, returned, y_in, mod, following, tout, qkv, out, kept_in,
    y, g, kept, x_v, sem,
):
    inside, video, slot = place_of(flags, per_core, late)

    @pl.when(inside)
    def _():
        leaving = (y_in[...] + mod[video][5:6] * dot(returned[...], tout[...])).astype(BF16)
        x_v[...] = leaving
        store = pltpu.make_async_copy(x_v, kept.at[slot], sem)
        store.start()
        spatial_part(leaving.astype(F32), following[video], qkv, out, y, g)
        store.wait()


def tail_kernel(per_core, flags, returned, y_in, mod, tout, kept_in, kept, x_v, sem):
    inside, video, slot = place_of(flags, per_core)

    @pl.when(inside)
    def _():
        leaving = (y_in[...] + mod[video][5:6] * dot(returned[...], tout[...])).astype(BF16)
        x_v[...] = leaving
        store = pltpu.make_async_copy(x_v, kept.at[slot], sem)
        store.start()
        store.wait()


SMEM = pl.BlockSpec(memory_space=pltpu.SMEM)
VMEM = pl.BlockSpec(memory_space=pltpu.VMEM)
ANY = pl.BlockSpec(memory_space=pl.ANY)
HBM = pl.BlockSpec(memory_space=pltpu.HBM)


def call(kernel, name, ins, outs, specs, scratch, aliases={}, limit=14, flops=0):
    return pl.pallas_call(
        kernel,
        name=name,
        in_specs=ins,
        out_specs=specs,
        out_shape=outs,
        scratch_shapes=scratch,
        input_output_aliases=aliases,
        cost_estimate=None if not flops else pl.CostEstimate(
            flops=flops, transcendentals=0, bytes_accessed=flops // 1000
        ),
        compiler_params=pltpu.CompilerParams(vmem_limit_bytes=limit * 2**20),
    )


def on_device(frames_in, spatial_qkv, spatial_out, temporal_qkv, temporal_out, modulation):
    videos, frames, patches, model = frames_in.shape
    wide, hw = spatial_qkv.shape[2], spatial_out.shape[1]
    per_core = videos // 2
    sections = lax.axis_size("section")
    ranks = lax.axis_size("seq")
    stages = sections // 2
    section = lax.axis_index("section")
    stage, core = section // 2, section % 2
    tokens = frames * patches
    share = patches // ranks
    columns = wide + padded(hw) - hw

    def swapped(a):
        return lax.ppermute(a, "section", [(i, i ^ 1) for i in range(sections)])

    shape = jax.ShapeDtypeStruct
    qkv_s, out_s = shape((model, columns), BF16), shape((hw, model), BF16)
    prepare = call(
        prepare_kernel, "prepare", [SMEM] + [HBM] * 4, [qkv_s] * 2 + [out_s] * 2,
        [ANY] * 2 + [VMEM] * 2,
        [pltpu.VMEM((columns, model), BF16)] * 2 + [pltpu.VMEM((model, columns), BF16)] * 2
        + [pltpu.SemaphoreType.DMA((2, 6))],
        limit=60,
    )
    chain = (stage + core) % 2
    core_id = core.reshape(1).astype(jnp.int32)
    flags = jnp.stack([stage, chain, jnp.zeros_like(stage)]).astype(jnp.int32)
    def prepared(qkv, out, qkv2, out2):
        return prepare(
            core_id, jnp.swapaxes(qkv[0], 0, 1), jnp.swapaxes(qkv2[0], 0, 1), out[0], out2[0]
        )

    mod = modulation[0]
    mod2, sqkv2, sout2 = swapped(mod), swapped(spatial_qkv), swapped(spatial_out)
    tqkv, tout, mod2, sqkv2, sout2 = lax.optimization_barrier(
        (temporal_qkv, temporal_out, mod2, sqkv2, sout2)
    )
    mod_e, mod_o = jnp.where(core == 0, mod, mod2), jnp.where(core == 0, mod2, mod)
    tqkv2, tout2 = swapped(tqkv), swapped(tout)
    sqkv_e, sqkv_o, sout_e, sout_o = prepared(spatial_qkv, spatial_out, sqkv2, sout2)
    source = frames_in.reshape(videos, tokens, model)

    x_s, y_s = shape((tokens, model), BF16), shape((tokens, model), F32)
    kept_s = shape((per_core, tokens, model), BF16)
    hold = [pltpu.VMEM((tokens, model), BF16), pltpu.SemaphoreType.DMA]
    at_s = shape((3,), jnp.int32)
    tick = call(
        tick_kernel, "tick", [SMEM, ANY], [at_s, x_s], [SMEM, ANY], [], {1: 1},
        flops=2 * 10**9,
    )
    first = call(
        functools.partial(first_kernel, per_core), "first", [SMEM] + [VMEM] * 4, [y_s, x_s],
        [VMEM, VMEM], [],
    )
    cross = call(
        functools.partial(cross_kernel, per_core, stages), "cross",
        [SMEM] + [VMEM] * 7 + [ANY, ANY], [y_s, x_s, kept_s], [VMEM, VMEM, ANY],
        [pltpu.VMEM((tokens, model), BF16)] * 2 + [pltpu.SemaphoreType.DMA((2,))], {9: 2},
        flops=0,
    )
    temporal = call(
        functools.partial(temporal_kernel, share), "temporal", [VMEM, VMEM], shape((tokens, hw), BF16), VMEM, [], flops=0,
    )
    joint = lambda late: call(
        functools.partial(joint_kernel, per_core, late), "joint",
        [SMEM] + [VMEM] * 7 + [ANY], [y_s, x_s, kept_s], [VMEM, VMEM, ANY], hold, {8: 2}, flops=0,
    )
    tail = call(
        functools.partial(tail_kernel, per_core), "tail",
        [SMEM] + [VMEM] * 4 + [ANY], [kept_s], [ANY], hold, {5: 0},
    )

    def exchange(a):
        out = lax.all_to_all(a.reshape(ranks, share, a.shape[1]), "seq", 0, 0, tiled=True)
        return out.reshape(a.shape)

    def sections_of(late, flags, even, y, g):
        mixed = temporal(exchange(g), tqkv_e)
        y, g, even = joint(late)(
            flags, exchange(mixed), y, mod_e, mod_o, tout_e, sqkv_o, sout_o, even
        )
        return even, y, g

    onward = [(i, ((i + 2) % sections) ^ 1) for i in range(sections)]
    back = [(j, i) for i, j in onward]

    def advance(carried):
        flags, even, odd, y, g = carried
        following, g = tick(flags, g)
        even, y, g = sections_of(1, following, even, y, g)
        y = lax.ppermute(y, "section", onward)
        mixed = lax.ppermute(temporal(exchange(g), tqkv_o), "section", onward)
        y, g, odd = cross(
            following, exchange(mixed), y, mod_p, mod_e, tout_p, sqkv_e, sout_e, source, odd
        )
        return following, even, odd, y, g

    kept = jnp.zeros(kept_s.shape, BF16)
    last = stages + per_core - 2
    y, g = first(flags, source, mod_e, sqkv_e, sout_e)
    before = [(i, (i + 2) % sections) for i in range(1, sections, 2)]
    tout_p = lax.ppermute(temporal_out[0], "section", before)
    mod_p = lax.ppermute(mod_o, "section", [(i, (i + 2) % sections) for i in range(sections)])
    tqkv2, g, tout_p, mod_p = lax.optimization_barrier((tqkv2, g, tout_p, mod_p))
    tout_p2 = lax.ppermute(tout_p, "section", [(i, i - 1) for i in range(1, sections, 2)])
    tqkv_e, tqkv_o, tout_e, tout_o = prepared(tqkv, tout, tqkv2, tout2)
    tout_p2, tout_o = lax.optimization_barrier((tout_p2, tout_o))
    tout_p = jnp.where(core == 0, tout_p2, tout_p)
    flags, even, odd, y, g = lax.while_loop(
        lambda carried: carried[0][2] < last, advance, (flags, kept, kept, y, g)
    )
    odd = lax.ppermute(odd, "section", back)
    even, y, g = sections_of(0, flags, even, y, g)
    mixed = temporal(exchange(g), tqkv_o)
    (odd,) = tail(flags, exchange(mixed), y, mod_o, tout_o, odd)
    own = jnp.where(core == 0, even, odd)
    other = swapped(jnp.where(core == 0, odd, even))
    low, high = jnp.where(chain == 0, own, other), jnp.where(chain == 0, other, own)
    hidden = jnp.concatenate([low, high], axis=0)
    return hidden.reshape((1,) + frames_in.shape)


def solution(mesh):
    placed = (
        P(None, "seq", None, None),
        P("section", None, None),
        P("section", None, None),
        P("section", None, None),
        P("section", None, None),
        P("section", None, None, None),
    )
    return jax.shard_map(
        on_device,
        mesh=mesh,
        in_specs=placed,
        out_specs=P("section", None, "seq", None, None),
        check_vma=False,
    )
```

```python
import functools

import jax
import jax.numpy as jnp
from jax import lax
from jax.experimental import pallas as pl
from jax.experimental.pallas import tpu as pltpu
from jax.sharding import PartitionSpec as P

HEADS = 8
LANES = 128
F32 = jnp.float32
BF16 = jnp.bfloat16
EPS = 1e-06


def padded(n):
    return -(-n // LANES) * LANES


def dot(a, b):
    return lax.dot_general(a, b, (((1,), (0,)), ((), ())), preferred_element_type=F32)


def dot_t(a, b):
    return lax.dot_general(a, b, (((1,), (1,)), ((), ())), preferred_element_type=F32)


def split(a):
    high = a.astype(BF16)
    return high, (a - high.astype(F32)).astype(BF16)


def norm_modulate(x, offset, scaling):
    average = jnp.mean(x, axis=-1, keepdims=True)
    centered = x - average
    variance = jnp.mean(centered * centered, axis=-1, keepdims=True)
    return (centered * lax.rsqrt(variance + EPS) * (1.0 + scaling) + offset).astype(BF16)


def in_head(shape, axis, start, head, width):
    at = lax.broadcasted_iota(jnp.int32, shape, axis) + start
    return jnp.logical_and(at >= head * width, at < (head + 1) * width)


def head_members(hw, width):
    row = lax.broadcasted_iota(jnp.int32, (hw, LANES), 0)
    col = lax.broadcasted_iota(jnp.int32, (hw, LANES), 1) * width
    tall = jnp.where(jnp.logical_and(row >= col, row < col + width), 1.0, 0.0)
    row = lax.broadcasted_iota(jnp.int32, (HEADS, hw), 0) * width
    col = lax.broadcasted_iota(jnp.int32, (HEADS, hw), 1)
    flat = jnp.where(jnp.logical_and(col >= row, col < row + width), 1.0, 0.0)
    return tall.astype(BF16), flat.astype(BF16)


def attention(projected, hw, patches):
    tokens = projected.shape[0]
    width = hw // HEADS
    begin = padded(hw)
    tall, flat = head_members(hw, width)
    queries, lookups = projected[:, :hw], projected[:, begin : begin + hw]
    values = projected[:, begin + hw : begin + 2 * hw].astype(BF16)
    high, low = split(queries * queries)
    rows = lax.rsqrt((dot(high, tall) + dot(low, tall)) * (1.0 / width) + EPS) * width**-0.5
    high, low = split(lookups * lookups)
    cols = lax.rsqrt((dot_t(flat, high) + dot_t(flat, low)) * (1.0 / width) + EPS)
    queries, lookups = queries.astype(BF16), lookups.astype(BF16)
    spans, scores = [], []
    for head in range(HEADS):
        first = head * width // LANES
        last = ((head + 1) * width - 1) // LANES
        start, stop = first * LANES, min((last + 1) * LANES, hw)
        mine = in_head((1, stop - start), 1, start, head, width)
        window = jnp.where(mine, queries[:, start:stop], jnp.zeros((), BF16))
        scores.append(dot_t(window, lookups[:, start:stop]))
        spans.append((first, last, start, stop))
    e = [jnp.exp(s * rows[:, h : h + 1] * cols[h : h + 1]) for h, s in enumerate(scores)]
    if patches:
        r = lax.broadcasted_iota(jnp.int32, (tokens, tokens), 0) % patches
        c = lax.broadcasted_iota(jnp.int32, (tokens, tokens), 1) % patches
        same = r == c
        e = [jnp.where(same, a, 0.0) for a in e]
    mixed = [dot(a.astype(BF16), values[:, s[2] : s[3]]) for a, s in zip(e, spans)]
    inverse = [1.0 / jnp.sum(a, axis=-1, keepdims=True) for a in e]
    tiles = [0.0] * (padded(hw) // LANES)
    for head, (first, last, start, stop) in enumerate(spans):
        result = mixed[head] * inverse[head]
        for tile in range(first, last + 1):
            left, right = tile * LANES, min(tile * LANES + LANES, hw)
            own = in_head((1, right - left), 1, left, head, width)
            tiles[tile] = jnp.where(own, result[:, left - start : right - start], tiles[tile])
    return jnp.concatenate(tiles, axis=1).astype(BF16)


def prepare_kernel(core, qkv, qkv2, out, out2, even, odd, out_e, out_o, *refs):
    turned, done, sems = refs[:2], refs[2:4], refs[4]
    hw, model = out.shape
    gap = padded(hw) - hw
    parts = ((0, 0, hw), (hw, hw + gap, hw), (2 * hw, 2 * hw + gap, hw))

    def piece(k, q, j):
        at, to, rows = parts[j]
        return pltpu.make_async_copy(
            q.at[pl.ds(at, rows)], turned[k].at[pl.ds(to, rows)], sems.at[k, j]
        )

    def begin(k, q, o):
        for j in range(len(parts)):
            piece(k, q, j).start()
        pltpu.make_async_copy(o, (out_e, out_o)[k], sems.at[k, 3]).start()

    for k in range(2):
        pick = core[0] if k == 0 else 1 - core[0]
        pl.when(pick == 0)(functools.partial(begin, k, qkv, out))
        pl.when(pick != 0)(functools.partial(begin, k, qkv2, out2))
        turned[k][hw : hw + gap, :] = jnp.zeros((gap, model), BF16)
    columns = turned[0].shape[0]
    halves = ((0, columns // 2 // LANES * LANES), (columns // 2 // LANES * LANES, columns))
    back = []
    for k in range(2):
        arrived = 0
        for n, (low, high) in enumerate(halves):
            while arrived < len(parts) and parts[arrived][1] < high:
                piece(k, qkv, arrived).wait()
                arrived += 1
            for j in range(low, high, LANES):
                done[k][:, j : j + LANES] = turned[k][j : j + LANES, :].T
            back.append(
                pltpu.make_async_copy(
                    done[k].at[:, pl.ds(low, high - low)],
                    (even, odd)[k].at[:, pl.ds(low, high - low)],
                    sems.at[k, 4 + n],
                )
            )
            back[-1].start()
    for k in range(2):
        pltpu.make_async_copy(out, (out_e, out_o)[k], sems.at[k, 3]).wait()
    for copy in back:
        copy.wait()


def place_of(flags, per_core, late=0):
    micro = flags[2] - late - flags[0]
    inside = jnp.logical_and(micro >= 0, micro < per_core)
    clipped = jnp.clip(micro, 0, per_core - 1)
    return inside, flags[1] * per_core + clipped, clipped


def spatial_part(x, factors, qkv, out, y, g, ready=None):
    normed = norm_modulate(x, factors[0:1], factors[1:2])
    if ready is not None:
        ready()
    mixed = attention(dot(normed, qkv[...]), out.shape[0], 0)
    middle = x + factors[2:3] * dot(mixed, out[...])
    y[...] = middle
    g[...] = norm_modulate(middle, factors[3:4], factors[4:5])


def tick_kernel(flags, g_in, following, after, g):
    following[0] = flags[0]
    following[1] = flags[1]
    following[2] = flags[2] + 1
    after[0] = flags[2] + 1


def first_kernel(per_core, flags, frames, mod, qkv, out, y, g):
    video = flags[1] * per_core

    @pl.when(flags[0] == 0)
    def _():
        spatial_part(frames[video].astype(F32), mod[video], qkv, out, y, g)


def cross_kernel(
    per_core, stages, flags, returned, y_in, mod_p, mod, tout_p, qkv, out, frames, kept_in,
    y, g, kept, x_v, new_v, sems,
):
    inside, video, _ = place_of(flags, per_core)
    micro = jnp.where(flags[0] == 0, flags[2] - stages, flags[2] - flags[0])
    finishing = jnp.logical_and(micro >= 0, micro < per_core)
    slot = jnp.clip(micro, 0, per_core - 1)

    @pl.when(finishing)
    def _():
        factor = mod_p[flags[1] * per_core + slot][5:6]
        x_v[...] = (y_in[...] + factor * dot(returned[...], tout_p[...])).astype(BF16)
        pltpu.make_async_copy(x_v, kept.at[slot], sems.at[0]).start()

    @pl.when(inside)
    def _():
        @pl.when(flags[0] == 0)
        def _():
            copy = pltpu.make_async_copy(frames.at[video], new_v, sems.at[1])
            copy.start()
            copy.wait()

        x = jnp.where(flags[0] == 0, new_v[...], x_v[...])
        spatial_part(x.astype(F32), mod[video], qkv, out, y, g)

    @pl.when(finishing)
    def _():
        pltpu.make_async_copy(x_v, kept.at[slot], sems.at[0]).wait()


def temporal_kernel(share, arrived, qkv, mixed):
    mixed[...] = attention(dot(arrived[...], qkv[...]), mixed.shape[1], share)


def joint_kernel(
    per_core, late, flags, returned, y_in, mod, following, tout, qkv, out, kept_in,
    y, g, kept, x_v, sem,
):
    inside, video, slot = place_of(flags, per_core, late)

    @pl.when(inside)
    def _():
        leaving = (y_in[...] + mod[video][5:6] * dot(returned[...], tout[...])).astype(BF16)
        x_v[...] = leaving
        store = pltpu.make_async_copy(x_v, kept.at[slot], sem)
        store.start()
        spatial_part(leaving.astype(F32), following[video], qkv, out, y, g)
        store.wait()


def tail_kernel(per_core, flags, returned, y_in, mod, tout, kept_in, kept, x_v, sem):
    inside, video, slot = place_of(flags, per_core)

    @pl.when(inside)
    def _():
        leaving = (y_in[...] + mod[video][5:6] * dot(returned[...], tout[...])).astype(BF16)
        x_v[...] = leaving
        store = pltpu.make_async_copy(x_v, kept.at[slot], sem)
        store.start()
        store.wait()


SMEM = pl.BlockSpec(memory_space=pltpu.SMEM)
VMEM = pl.BlockSpec(memory_space=pltpu.VMEM)
ANY = pl.BlockSpec(memory_space=pl.ANY)
HBM = pl.BlockSpec(memory_space=pltpu.HBM)


def call(kernel, name, ins, outs, specs, scratch, aliases={}, limit=14, flops=0):
    return pl.pallas_call(
        kernel,
        name=name,
        in_specs=ins,
        out_specs=specs,
        out_shape=outs,
        scratch_shapes=scratch,
        input_output_aliases=aliases,
        cost_estimate=None if not flops else pl.CostEstimate(
            flops=flops, transcendentals=0, bytes_accessed=flops // 1000
        ),
        compiler_params=pltpu.CompilerParams(vmem_limit_bytes=limit * 2**20),
    )


def on_device(frames_in, spatial_qkv, spatial_out, temporal_qkv, temporal_out, modulation):
    videos, frames, patches, model = frames_in.shape
    wide, hw = spatial_qkv.shape[2], spatial_out.shape[1]
    per_core = videos // 2
    sections = lax.axis_size("section")
    ranks = lax.axis_size("seq")
    stages = sections // 2
    section = lax.axis_index("section")
    stage, core = section // 2, section % 2
    tokens = frames * patches
    share = patches // ranks
    columns = wide + padded(hw) - hw

    def swapped(a):
        return lax.ppermute(a, "section", [(i, i ^ 1) for i in range(sections)])

    shape = jax.ShapeDtypeStruct
    qkv_s, out_s = shape((model, columns), BF16), shape((hw, model), BF16)
    prepare = call(
        prepare_kernel, "prepare", [SMEM] + [HBM] * 4, [qkv_s] * 2 + [out_s] * 2,
        [ANY] * 2 + [VMEM] * 2,
        [pltpu.VMEM((columns, model), BF16)] * 2 + [pltpu.VMEM((model, columns), BF16)] * 2
        + [pltpu.SemaphoreType.DMA((2, 6))],
        limit=60,
    )
    chain = (stage + core) % 2
    core_id = core.reshape(1).astype(jnp.int32)
    flags = jnp.stack([stage, chain, jnp.zeros_like(stage)]).astype(jnp.int32)
    def prepared(qkv, out, qkv2, out2):
        return prepare(
            core_id, jnp.swapaxes(qkv[0], 0, 1), jnp.swapaxes(qkv2[0], 0, 1), out[0], out2[0]
        )

    mod = modulation[0]
    mod2, sqkv2, sout2 = swapped(mod), swapped(spatial_qkv), swapped(spatial_out)
    tqkv, tout, mod2, sqkv2, sout2 = lax.optimization_barrier(
        (temporal_qkv, temporal_out, mod2, sqkv2, sout2)
    )
    mod_e, mod_o = jnp.where(core == 0, mod, mod2), jnp.where(core == 0, mod2, mod)
    tqkv2, tout2 = swapped(tqkv), swapped(tout)
    sqkv_e, sqkv_o, sout_e, sout_o = prepared(spatial_qkv, spatial_out, sqkv2, sout2)
    source = frames_in.reshape(videos, tokens, model)

    x_s, y_s = shape((tokens, model), BF16), shape((tokens, model), F32)
    kept_s = shape((per_core, tokens, model), BF16)
    hold = [pltpu.VMEM((tokens, model), BF16), pltpu.SemaphoreType.DMA]
    one_s, at_s = shape((1,), jnp.int32), shape((3,), jnp.int32)
    tick = call(
        tick_kernel, "tick", [SMEM, ANY], [at_s, one_s, x_s], [SMEM, SMEM, ANY], [], {1: 2},
        flops=2 * 10**9,
    )
    first = call(
        functools.partial(first_kernel, per_core), "first", [SMEM] + [VMEM] * 4, [y_s, x_s],
        [VMEM, VMEM], [],
    )
    cross = call(
        functools.partial(cross_kernel, per_core, stages), "cross",
        [SMEM] + [VMEM] * 7 + [ANY, ANY], [y_s, x_s, kept_s], [VMEM, VMEM, ANY],
        [pltpu.VMEM((tokens, model), BF16)] * 2 + [pltpu.SemaphoreType.DMA((2,))], {9: 2},
        flops=0,
    )
    temporal = call(
        functools.partial(temporal_kernel, share), "temporal", [VMEM, VMEM], shape((tokens, hw), BF16), VMEM, [], flops=0,
    )
    joint = lambda late: call(
        functools.partial(joint_kernel, per_core, late), "joint",
        [SMEM] + [VMEM] * 7 + [ANY], [y_s, x_s, kept_s], [VMEM, VMEM, ANY], hold, {8: 2}, flops=0,
    )
    tail = call(
        functools.partial(tail_kernel, per_core), "tail",
        [SMEM] + [VMEM] * 4 + [ANY], [kept_s], [ANY], hold, {5: 0},
    )

    def exchange(a):
        out = lax.all_to_all(a.reshape(ranks, share, a.shape[1]), "seq", 0, 0, tiled=True)
        return out.reshape(a.shape)

    def sections_of(late, flags, even, y, g):
        mixed = temporal(exchange(g), tqkv_e)
        y, g, even = joint(late)(
            flags, exchange(mixed), y, mod_e, mod_o, tout_e, sqkv_o, sout_o, even
        )
        return even, y, g

    onward = [(i, ((i + 2) % sections) ^ 1) for i in range(sections)]
    back = [(j, i) for i, j in onward]

    def advance(carried):
        _, flags, even, odd, y, g = carried
        following, after, g = tick(flags, g)
        even, y, g = sections_of(1, following, even, y, g)
        y = lax.ppermute(y, "section", onward)
        mixed = lax.ppermute(temporal(exchange(g), tqkv_o), "section", onward)
        y, g, odd = cross(
            following, exchange(mixed), y, mod_p, mod_e, tout_p, sqkv_e, sout_e, source, odd
        )
        return after, following, even, odd, y, g

    kept = jnp.zeros(kept_s.shape, BF16)
    last = stages + per_core - 2
    y, g = first(flags, source, mod_e, sqkv_e, sout_e)
    before = [(i, (i + 2) % sections) for i in range(1, sections, 2)]
    tout_p = lax.ppermute(temporal_out[0], "section", before)
    mod_p = lax.ppermute(mod_o, "section", [(i, (i + 2) % sections) for i in range(sections)])
    tqkv2, g, tout_p, mod_p = lax.optimization_barrier((tqkv2, g, tout_p, mod_p))
    tout_p2 = lax.ppermute(tout_p, "section", [(i, i - 1) for i in range(1, sections, 2)])
    tqkv_e, tqkv_o, tout_e, tout_o = prepared(tqkv, tout, tqkv2, tout2)
    tout_p2, tout_o = lax.optimization_barrier((tout_p2, tout_o))
    tout_p = jnp.where(core == 0, tout_p2, tout_p)
    start = jnp.zeros((1,), jnp.int32)
    _, flags, even, odd, y, g = lax.while_loop(
        lambda carried: carried[0][0] < last, advance, (start, flags, kept, kept, y, g)
    )
    odd = lax.ppermute(odd, "section", back)
    even, y, g = sections_of(0, flags, even, y, g)
    mixed = temporal(exchange(g), tqkv_o)
    (odd,) = tail(flags, exchange(mixed), y, mod_o, tout_o, odd)
    own = jnp.where(core == 0, even, odd)
    other = swapped(jnp.where(core == 0, odd, even))
    low, high = jnp.where(chain == 0, own, other), jnp.where(chain == 0, other, own)
    hidden = jnp.concatenate([low, high], axis=0)
    return hidden.reshape((1,) + frames_in.shape)


def solution(mesh):
    placed = (
        P(None, "seq", None, None),
        P("section", None, None),
        P("section", None, None),
        P("section", None, None),
        P("section", None, None),
        P("section", None, None, None),
    )
    return jax.shard_map(
        on_device,
        mesh=mesh,
        in_specs=placed,
        out_specs=P("section", None, "seq", None, None),
        check_vma=False,
    )
```
